32 devices in a mesh: dp: 8 (over z, x), mp: 4 (over y, core).
Axes of the slice: x: 2, y: 2, z: 4, core: 2. Of those that a mesh axis runs over, the one named last changes fastest.
Arguments:
- inputs: float32 [8, 1024, 1536], P('dp', 'mp'), may hold values from -6 to 6
- segments: int32 [8, 1024], P('dp'), may hold values from 0 to 7, never falling along the last dimension, each value on 1 to 512 neighbouring positions
- attend_gain: float32 [1536], P(('dp', 'mp')), may hold values from 0.1 to 1.9
- feed_gain: float32 [1536], P(('dp', 'mp')), may hold values from 0.1 to 1.9
- w_query: float32 [1536, 768], P('dp', 'mp'), may hold values from -0.01953125 to 0.01953125
- w_key: float32 [1536, 768], P('dp', 'mp'), may hold values from -0.15625 to 0.15625
- w_value: float32 [1536, 768], P('dp', 'mp'), may hold values from -0.15625 to 0.15625
- w_mixer: float32 [768, 1536], P('mp', 'dp'), may hold values from -0.875 to 0.875
- rel_table: float32 [32, 12], P(None, 'mp'), may hold values from -4 to 4
- w_gate: float32 [1536, 3968], P('dp', 'mp'), may hold values from -0.15625 to 0.15625
- w_lift: float32 [1536, 3968], P('dp', 'mp'), may hold values from -0.15625 to 0.15625
- w_down: float32 [3968, 1536], P('mp', 'dp'), may hold values from -0.09375 to 0.09375
- cotangent: float32 [8, 1024, 1536], P('dp', 'mp'), may hold values from -6 to 6
Outputs:
- output: float32 [8, 1024, 1536], P('dp', 'mp')
- input_grad: float32 [8, 1024, 1536], P('dp', 'mp')
- attend_grad: float32 [1536], P(('dp', 'mp'))
- feed_grad: float32 [1536], P(('dp', 'mp'))
- query_grad: float32 [1536, 768], P('dp', 'mp')
- key_grad: float32 [1536, 768], P('dp', 'mp')
- value_grad: float32 [1536, 768], P('dp', 'mp')
- mixer_grad: float32 [768, 1536], P('mp', 'dp')
- table_grad: float32 [32, 12], P(None, 'mp')
- gate_grad: float32 [1536, 3968], P('dp', 'mp')
- lift_grad: float32 [1536, 3968], P('dp', 'mp')
- down_grad: float32 [3968, 1536], P('mp', 'dp')
The draws below stay inside these ranges and needn't reach their ends.
Inputs may be any that keep to these rules, and one draw needn't show every extreme that they name: `segments`: in each row the segment ids never fall, and each id covers between 1 and 512 consecutive positions; one covers exactly 512.
All inputs are finite; a program needn't handle non-finite values.
Results may differ from the reference program's by a relative error of at most 0.013.
The reference program's roundings to bfloat16 on the way count: a program that leaves them out, or rounds other values in their place, can miss the bound.
Values may be sent and summed in bfloat16 or wider, within the bound.
A program may use at most 192 MiB of HBM per device.

```python
import math
import jax
import jax.numpy as jnp
import numpy as np
from jax import lax

D = 1536
HEADS = 12
HEAD_DIM = 64
FF = 3968
BUCKETS = 32
LEN = 1024
ROWS = 8


def spiked(values, stream_key, source, target, shards_of, factor):
    owner, partner = [(jnp.arange(values.shape[axis_at]) // (values.shape[axis_at] // shards_of)).reshape([-1 if axis == axis_at else 1 for axis in range(values.ndim)]) for axis_at in (source, target)]
    chosen = jax.random.permutation(stream_key, shards_of)[partner]
    strong = (owner == chosen) | (owner == (partner + shards_of // 2) % shards_of)
    return jnp.where(strong, factor * values, values)


def levels(own_key, shape, cuts, low, largest):
    loudness, own = 1.0, jax.random.fold_in(own_key, 6)
    for dim, blocks in cuts:
        draws = jnp.exp(jax.random.uniform(jax.random.fold_in(own, dim), (blocks,), jnp.float32, low / len(cuts), largest / len(cuts)))
        loudness = loudness * jnp.repeat(draws, shape[dim] // blocks).reshape([-1 if axis == dim else 1 for axis in range(len(shape))])
    return loudness


def length_profile(count, total, most, slope):
    weights = [(1 << 20) // math.isqrt(rank ** slope) + 1 for rank in range(2, count + 1)]
    rest, given = total - most - (count - 1), [1] * (count - 1)
    while rest > 0:
        free = [i for i in range(count - 1) if given[i] < most]
        whole, remaining = sum([weights[i] for i in free]), rest
        for i in free:
            more = min(most - given[i], max(1, remaining * weights[i] // whole), rest)
            given[i] = given[i] + more
            rest = rest - more
    return np.array([most] + given)


def ragged(own_key, amount, total, reach, lean):
    if amount == 2:
        one = jax.random.randint(own_key, (), max(1, total - reach), min(reach, total - 1) + 1)
        return jnp.stack([one, total - one])
    sizes = jnp.asarray(length_profile(amount, total, reach, lean), jnp.int32)
    pairs = (amount - 1) // 2
    giver, sink = sizes[1:1 + 2 * pairs:2], sizes[2:2 + 2 * pairs:2]
    slack = jnp.minimum(giver - 1, reach - sink)
    moved = jax.random.randint(jax.random.fold_in(own_key, 1), (pairs,), 0, 1 << 20) % (slack + 1)
    sizes = sizes.at[1:1 + 2 * pairs:2].set(giver - moved).at[2:2 + 2 * pairs:2].set(sink + moved)
    return sizes[jax.random.permutation(jax.random.fold_in(own_key, 2), amount)]


def scatter_about(stream_key, extent, scale, most, cuts=(), held_as=jnp.bfloat16):
    factor_of = levels(stream_key, extent, cuts, -0.22, 0.18) if cuts else 1.0
    entries = jax.random.normal(stream_key, extent, jnp.float32) * scale * factor_of
    return jnp.minimum(jnp.maximum(entries, -most), most).astype(held_as)


def heavy_noise(key, extent, scale, bound, split, heavy, kind=jnp.bfloat16):
    array = scale * jax.random.normal(key, extent, jnp.float32)
    if split:
        array = array * levels(key, extent, split, -0.22, 0.18)
    return jnp.clip(spiked(array, jax.random.fold_in(key, 3), *heavy), -bound, bound).astype(kind)


def setup_inputs(seed: int = 0) -> dict:
    arg_keys = jax.random.split(jax.random.key(seed), 14)
    inputs = heavy_noise(arg_keys[0], (ROWS, LEN, D), 1.0, 6.0, ((0, 8), (1, 4)), (0, 2, 8, 2.0), jnp.float32)
    segments = jax.vmap(lambda own: jnp.searchsorted(jnp.cumsum(ragged(own, 8, LEN, LEN // 2, 0)), jnp.arange(LEN), side="right"))(jax.random.split(arg_keys[1], ROWS)).reshape((ROWS, LEN)).astype(jnp.int32)
    attend_gain = jnp.clip(1.0 + 0.18 * jax.random.normal(arg_keys[2], (D,), jnp.float32), 0.1, 1.9)
    feed_gain = jnp.clip(1.0 + 0.18 * jax.random.normal(arg_keys[3], (D,), jnp.float32), 0.1, 1.9)
    w_query = scatter_about(arg_keys[4], (D, HEADS * HEAD_DIM), (D * HEAD_DIM) ** -0.5, 0.01953125, ((0, 8), (1, 4)), jnp.float32)
    w_key = scatter_about(arg_keys[5], (D, HEADS * HEAD_DIM), D ** -0.5, 0.15625, ((0, 8), (1, 4)), jnp.float32)
    w_value = scatter_about(arg_keys[6], (D, HEADS * HEAD_DIM), D ** -0.5, 0.15625, ((0, 8), (1, 4)), jnp.float32)
    w_mixer = scatter_about(arg_keys[7], (HEADS * HEAD_DIM, D), (HEADS * HEAD_DIM // 16) ** -0.5, 0.875, ((0, 4), (1, 8)), jnp.float32)
    rel_table = scatter_about(arg_keys[8], (BUCKETS, HEADS), 1.0, 4.0, ((1, 4),), jnp.float32)
    w_gate = scatter_about(arg_keys[9], (D, FF), D ** -0.5, 0.15625, ((0, 8), (1, 4)), jnp.float32)
    w_lift = scatter_about(arg_keys[10], (D, FF), D ** -0.5, 0.15625, ((0, 8), (1, 4)), jnp.float32)
    w_down = scatter_about(arg_keys[11], (FF, D), FF ** -0.5, 0.09375, ((0, 4), (1, 8)), jnp.float32)
    cotangent = heavy_noise(arg_keys[12], (ROWS, LEN, D), 1.0, 6.0, ((0, 8), (1, 4)), (0, 2, 8, 2.0), jnp.float32)
    return dict(inputs=inputs, segments=segments, attend_gain=attend_gain, feed_gain=feed_gain, w_query=w_query, w_key=w_key, w_value=w_value, w_mixer=w_mixer, rel_table=rel_table, w_gate=w_gate, w_lift=w_lift, w_down=w_down, cotangent=cotangent)


EPSILON = 1e-06
THRESHOLDS = (8, 12, 16, 23, 32, 46, 64, 91)
HIGHEST = lax.Precision.HIGHEST

@jax.custom_vjp
def low(v):
    return lax.optimization_barrier(v.astype(jnp.bfloat16)).astype(jnp.float32)

@jax.custom_vjp
def low_back(v):
    return v

def low_keep(v):
    return (low(v), None)

def low_pass(kept, grad):
    return (grad,)

def back_keep(v):
    return (v, None)

def back_low(kept, grad):
    return (low(grad),)
low.defvjp(low_keep, low_pass)
low_back.defvjp(back_keep, back_low)

def bucket_table(length):
    places = jnp.arange(length, dtype=jnp.int32)
    offset = places[None, :] - places[:, None]
    distance = jnp.abs(offset)
    far_bucket = 7 + sum(((distance >= limit).astype(jnp.int32) for limit in THRESHOLDS))
    near = jnp.where(distance < 8, distance, far_bucket).astype(jnp.int32)
    return near + jnp.where(offset > 0, 16, 0).astype(jnp.int32)

def rms_scaled(values, gain):
    return values * lax.rsqrt(lax.optimization_barrier(jnp.mean(values * values, axis=-1, keepdims=True)) + EPSILON) * gain

def project(left, weight):
    return jnp.einsum('rld,de->rle', left, weight, precision=HIGHEST)

def reference(inputs, segments, attend_gain, feed_gain, w_query, w_key, w_value, w_mixer, rel_table, w_gate, w_lift, w_down, cotangent):
    length = inputs.shape[1]
    heads = rel_table.shape[1]
    buckets = bucket_table(length)

    def forward(inputs, attend_gain, feed_gain, w_query, w_key, w_value, w_mixer, rel_table, w_gate, w_lift, w_down):
        bias = jnp.transpose(rel_table[buckets], (2, 0, 1))
        normed = low(rms_scaled(inputs, low(attend_gain)))
        query = low_back(low(project(normed, low(w_query))))
        keys = low_back(low(project(normed, low(w_key))))
        values = low_back(low(project(normed, low(w_value))))
        width = query.shape[-1] // heads

        def attend(row):
            query_row, key_row, value_row, segment_row = row
            query_heads = query_row.reshape(length, heads, width)
            key_heads = key_row.reshape(length, heads, width)
            value_heads = value_row.reshape(length, heads, width)
            scores = jnp.einsum('ihe,jhe->hij', query_heads, key_heads, precision=HIGHEST) + bias
            scores = low_back(scores)
            same = (segment_row[:, None] == segment_row[None, :])[None]
            scores = jnp.where(same, scores, -1e+30)
            probs = low(jax.nn.softmax(scores, axis=-1))
            context = jnp.einsum('hij,jhe->ihe', probs, value_heads, precision=HIGHEST)
            return context.reshape(length, heads * width)
        context = lax.map(jax.checkpoint(attend), (query, keys, values, segments))
        context = low_back(low(context))
        mixed = low_back(project(context, low(w_mixer)))
        middle = inputs + mixed
        normed_two = low(rms_scaled(middle, low(feed_gain)))
        gate = low_back(project(normed_two, low(w_gate)))
        lift = low_back(project(normed_two, low(w_lift)))
        hidden = low(jax.nn.gelu(gate, approximate=True) * lift)
        down = low_back(project(hidden, low(w_down)))
        return middle + down
    output, pullback = jax.vjp(forward, inputs, attend_gain, feed_gain, w_query, w_key, w_value, w_mixer, rel_table, w_gate, w_lift, w_down)
    grads = pullback(cotangent)
    return (output, grads[0], grads[1], grads[2], grads[3], grads[4], grads[5], grads[6], grads[7], grads[8], grads[9], grads[10])
```

```python
import functools

import jax
import jax.numpy as jnp
from jax import lax
from jax.experimental import pallas as pl
from jax.experimental.pallas import tpu as pltpu
from jax.sharding import PartitionSpec as P

EPSILON = 1e-06
MESH = pl.DeviceIdType.MESH
BF16 = jnp.bfloat16
F32 = jnp.float32
VMEM_SPEC = pl.BlockSpec(memory_space=pltpu.VMEM)
ANY_SPEC = pl.BlockSpec(memory_space=pl.ANY)
DMA = pltpu.SemaphoreType.DMA


def remote(source, target, send_sem, recv_sem, where):
    return pltpu.make_async_remote_copy(
        src_ref=source,
        dst_ref=target,
        send_sem=send_sem,
        recv_sem=recv_sem,
        device_id=where,
        device_id_type=MESH,
    )


def matmul(left, right):
    return lax.dot_general(left, right, (((1,), (0,)), ((), ())), preferred_element_type=F32)


def matmul_nt(left, right):
    return lax.dot_general(left, right, (((1,), (1,)), ((), ())), preferred_element_type=F32)


def matmul_tn(left, right):
    return lax.dot_general(left, right, (((0,), (0,)), ((), ())), preferred_element_type=F32)


class Place:
    def __init__(self, n):
        self.n = n
        self.d = lax.axis_index("dp")
        self.m = lax.axis_index("mp")
        self.pos = lax.rem(self.d, 2) * (n - 1) + (self.d // 2) * (1 - 2 * lax.rem(self.d, 2))
        self.right = self.device(self.pos + 1)
        self.left = self.device(self.pos + n - 1)
        self.mate = self.m + 1 - 2 * lax.rem(self.m, 2)
        self.twin = lax.rem(self.m + 2, 4)
        self.far = lax.rem(self.mate + 2, 4)

    def device(self, position):
        position = lax.rem(position, self.n)
        late = position // (self.n // 2)
        return 2 * position * (1 - late) + (2 * (self.n - 1 - position) + 1) * late

    def barrier(self, ring=True, pair=True, everyone=False):
        sem = pltpu.get_barrier_semaphore()
        partners = []
        if everyone:
            partners += [{"dp": lax.rem(self.d + k, self.n)} for k in range(1, self.n)]
        elif ring:
            partners += [{"dp": self.right}, {"dp": self.left}]
        if pair:
            partners += [{"mp": self.mate}, {"mp": self.twin}, {"mp": self.far}]
        for where in partners:
            pl.semaphore_signal(sem, inc=1, device_id=where, device_id_type=MESH)
        pl.semaphore_wait(sem, len(partners))


class RingGather:
    def __init__(self, place, full, send, recv):
        self.place, self.full, self.send, self.recv = place, full, send, recv
        self.steps = place.n // 2

    def part(self, way, position, step):
        slot = self.full.at[self.place.device(position + self.place.n)]
        if step < self.steps - 1:
            return slot
        half = self.full.shape[1] // 2
        return slot.at[pl.ds(half * way, half)]

    def outgoing(self, way, step):
        ref = self.part(way, self.place.pos + (step if way else -step), step)
        where = {"dp": self.place.left if way else self.place.right}
        return remote(ref, ref, self.send.at[way, step], self.recv.at[way, step], where)

    def incoming(self, way, step):
        ref = self.part(way, self.place.pos + (1 + step if way else -1 - step), step)
        where = {"dp": self.place.left if way else self.place.right}
        return remote(ref, ref, self.send.at[way, step], self.recv.at[way, step], where)

    def advance(self, way, step):
        if step:
            self.incoming(way, step - 1).wait_recv()
        if step < self.steps:
            self.outgoing(way, step).start()

    def finish(self):
        for way in (0, 1):
            for step in range(self.steps):
                self.outgoing(way, step).wait_send()


class PairGather:
    def __init__(self, place, full, send, recv, chunks=2):
        self.place, self.full, self.send, self.recv, self.chunks = place, full, send, recv, chunks

    def rows(self, owner, chunk):
        size = self.full.shape[0] // 4
        part = size // self.chunks
        return self.full.at[pl.ds(pl.multiple_of(owner * size + chunk * part, part), part)]

    def copy(self, kind, chunk, owner):
        where = {"mp": self.place.twin if kind == 1 else self.place.mate}
        ref = self.rows(owner, chunk)
        return remote(ref, ref, self.send.at[kind, chunk], self.recv.at[kind, chunk], where)

    def begin(self, chunk):
        self.copy(1, chunk, self.place.m).start()
        self.copy(0, chunk, self.place.m).start()

    def relay(self, chunk):
        self.copy(1, chunk, self.place.twin).wait_recv()
        self.copy(2, chunk, self.place.twin).start()

    def end(self, chunk):
        self.copy(0, chunk, self.place.mate).wait_recv()
        self.copy(2, chunk, self.place.far).wait_recv()
        for kind in range(3):
            self.copy(kind, chunk, self.place.m).wait_send()


def norm_scale(values):
    return lax.rsqrt(jnp.mean(values * values, axis=-1, keepdims=True) + EPSILON)


class PairScatter:
    def __init__(self, place, give, got, over, came, send, recv, chunks=2):
        self.place, self.chunks = place, chunks
        self.give, self.got, self.over, self.came = give, got, over, came
        self.send, self.recv = send, recv

    def rows(self, chunk):
        part = self.over.shape[0] // self.chunks
        return pl.ds(chunk * part, part)

    def copy(self, kind, chunk):
        rows = self.rows(chunk)
        if kind == 2:
            source, target, where = self.over.at[rows], self.came.at[rows], {"mp": self.place.twin}
        else:
            source, target, where = self.give.at[kind, rows], self.got.at[kind, rows], {"mp": self.place.mate}
        return remote(source, target, self.send.at[kind, chunk], self.recv.at[kind, chunk], where)

    def far(self, value):
        self.give[0] = value.astype(BF16)
        for chunk in range(self.chunks):
            self.copy(0, chunk).start()

    def twin(self, value):
        part = self.over.shape[0] // self.chunks
        for chunk in range(self.chunks):
            rows = self.rows(chunk)
            self.copy(0, chunk).wait_recv()
            mine = value[chunk * part : (chunk + 1) * part]
            self.over[rows, :] = (mine + self.got[0, rows, :].astype(F32)).astype(BF16)
            self.copy(2, chunk).start()

    def mate(self, value):
        self.give[1] = value.astype(BF16)
        for chunk in range(self.chunks):
            self.copy(1, chunk).start()

    def take(self, chunk, value):
        rows = self.rows(chunk)
        self.copy(1, chunk).wait_recv()
        self.copy(2, chunk).wait_recv()
        return value + self.got[1, rows, :].astype(F32) + self.came[rows, :].astype(F32)

    def finish(self):
        for kind in range(3):
            for chunk in range(self.chunks):
                self.copy(kind, chunk).wait_send()

    @staticmethod
    def scratch(rows, columns, chunks=2):
        return [
            pltpu.VMEM((2, rows, columns), BF16), pltpu.VMEM((2, rows, columns), BF16),
            pltpu.VMEM((rows, columns), BF16), pltpu.VMEM((rows, columns), BF16),
            DMA((3, chunks)), DMA((3, chunks)),
        ]


class RingScatter:
    def __init__(self, place, term, out, put, inbox, send, recv):
        self.place, self.term, self.out, self.put, self.inbox = place, term, out, put, inbox
        self.send, self.recv = send, recv
        self.steps = place.n // 2

    def copy(self, way, step):
        source, target = self.put.at[way, step], self.inbox.at[way, step]
        if step == 0:
            half = source.shape[0] // 2
            rows = pl.ds(half * way, half)
            source, target = source.at[rows], target.at[rows]
        where = {"dp": self.place.left if way else self.place.right}
        return remote(source, target, self.send.at[way, step], self.recv.at[way, step], where)

    def arrived(self, way, step, total):
        self.copy(way, step).wait_recv()
        if step:
            return total + self.inbox[way, step].astype(F32)
        half = total.shape[0] // 2
        if way:
            return jnp.concatenate([total[:half], total[half:] + self.inbox[way, 0, half:, :].astype(F32)], axis=0)
        return jnp.concatenate([total[:half] + self.inbox[way, 0, :half, :].astype(F32), total[half:]], axis=0)

    def advance(self, way, step):
        n = self.place.n
        away = self.steps - step
        owner = self.place.device(self.place.pos + (n - away if way else away))
        total = self.term(owner)
        if step:
            total = self.arrived(way, step - 1, total)
        self.put[way, step] = total.astype(BF16)
        self.copy(way, step).start()

    def finish(self):
        total = self.term(self.place.d)
        for way in (0, 1):
            total = self.arrived(way, self.steps - 1, total)
        self.out[...] = total
        for way in (0, 1):
            for step in range(self.steps):
                self.copy(way, step).wait_send()

    @staticmethod
    def scratch(n, rows, columns):
        return [
            pltpu.VMEM((2, n // 2, rows, columns), BF16), pltpu.VMEM((2, n // 2, rows, columns), BF16),
            DMA((2, n // 2)), DMA((2, n // 2)),
        ]


def slot_columns(ref, slot, n):
    width = ref.shape[1] // n
    pair = ref[:, pl.ds(pl.multiple_of((slot // 2) * (2 * width), 2 * width), 2 * width)]
    return jnp.where(lax.rem(slot, 2) == 0, pair[:, :width], pair[:, width:])


def gate_terms(gate):
    square = gate * gate
    inner = 0.7978845608 * (gate + 0.044715 * (square * gate))
    bend = jnp.tanh(inner)
    half = 0.5 * (1.0 + bend)
    slope = half + 0.5 * gate * (1.0 - bend * bend) * (0.7978845608 * (1.0 + 0.134145 * square))
    return gate * half, slope


def bias_tiles(row_ref, tiles_ref):
    heads, kinds, block, _ = tiles_ref.shape
    for h in range(heads):
        for t in range(kinds):
            line = jnp.broadcast_to(row_ref[pl.ds(h * kinds + t, 1), :], (block, 2 * block))
            if t in (0, kinds - 1):
                tiles_ref[h, t] = line[:, :block]
            else:
                tiles_ref[h, t] = pltpu.roll(line, 0, 1, stride=1, stride_axis=0)[:, :block]


def key_window(seg_smem, index, block, count):
    first, last = seg_smem[0, index * block], seg_smem[0, index * block + block - 1]
    low, high = jnp.int32(0), jnp.int32(0)
    for j in range(count):
        low += (seg_smem[0, j * block + block - 1] < first).astype(jnp.int32)
        high += (seg_smem[0, j * block] <= last).astype(jnp.int32)
    return low, high - low


def score_block(query, key_rows, tile, same):
    return jnp.where(same, matmul_nt(query, key_rows) + tile, -1e30)


def attend_kernel(seg_smem, qkv_ref, segr_ref, segc_ref, tiles_ref, ctx_ref, ctx32_ref, lse_ref):
    heads, _, block, _ = tiles_ref.shape
    length, width = qkv_ref.shape
    width = width // (3 * heads)
    count = length // block

    def run(index, low, blocks):
        rows = pl.ds(pl.multiple_of(index * block, block), block)
        seg_q = segc_ref[rows, :]
        places, sames, tile_at = [], [], []
        for t in range(blocks):
            j = low + t
            place = pl.ds(pl.multiple_of(j * block, block), block)
            places.append(place)
            sames.append(seg_q == segr_ref[:, place])
            tile_at.append(jnp.clip(j - index, -2, 2) + 2)
        outs, logs = [], []
        for h in range(heads):
            lanes = slice(h * width, (h + 1) * width)
            query = qkv_ref[rows, :][:, lanes]
            scores = []
            for t in range(blocks):
                key_rows = qkv_ref[places[t], :][:, heads * width + h * width : heads * width + (h + 1) * width]
                scores.append(score_block(query, key_rows, tiles_ref[h, tile_at[t]], sames[t]))
            peak = functools.reduce(jnp.maximum, scores)
            peak = jnp.max(peak, axis=1, keepdims=True)
            raised = [jnp.exp(s - peak) for s in scores]
            total = jnp.sum(functools.reduce(jnp.add, raised), axis=1, keepdims=True)
            scale = 1.0 / total
            context = jnp.zeros((block, width), F32)
            for t in range(blocks):
                value_rows = qkv_ref[places[t], :][:, 2 * heads * width + h * width : 2 * heads * width + (h + 1) * width]
                context += matmul((raised[t] * scale).astype(BF16), value_rows)
            outs.append(context)
            logs.append(peak + jnp.log(total))
        context = jnp.concatenate(outs, axis=1)
        ctx32_ref[rows, :] = context
        ctx_ref[rows, :] = context.astype(BF16)
        lse_ref[rows, :] = jnp.concatenate(logs + [jnp.zeros((block, 8 - heads), F32)], axis=1)

    @pl.loop(0, count)
    def _(index):
        low, many = key_window(seg_smem, index, block, count)
        for blocks in range(1, count + 1):
            pl.when(many == blocks)(functools.partial(run, index, low, blocks))


def attend(qkv, segments, tiles):
    length, width = qkv.shape
    heads = tiles.shape[0]
    return pl.pallas_call(
        attend_kernel,
        name="attend",
        out_shape=(
            jax.ShapeDtypeStruct((length, width // 3), BF16),
            jax.ShapeDtypeStruct((length, width // 3), F32),
            jax.ShapeDtypeStruct((length, 8), F32),
        ),
        in_specs=[pl.BlockSpec(memory_space=pltpu.SMEM)] + [VMEM_SPEC] * 4,
        out_specs=(VMEM_SPEC,) * 3,
    )(segments, qkv, segments, segments.reshape(length, 1), tiles)


def attend_back_kernel(
    seg_smem, qkv_ref, segr_ref, segc_ref, tiles_ref, ctx32_ref, lse_ref, mixed_ref, wmix_ref, buckets_ref,
    cots_ref, table_ref, do_ref, dk_ref, dv_ref, sums_ref,
):
    heads, kinds, block, _ = tiles_ref.shape
    length, width = qkv_ref.shape
    width = width // (3 * heads)
    count = length // block
    dk_ref[...] = jnp.zeros_like(dk_ref)
    dv_ref[...] = jnp.zeros_like(dv_ref)
    sums_ref[...] = jnp.zeros_like(sums_ref)

    @pl.loop(0, count)
    def _(index):
        rows = pl.ds(pl.multiple_of(index * block, block), block)
        weight = wmix_ref[...].reshape(-1, heads * width)
        do_ref[rows, :] = matmul(mixed_ref[rows, :], weight).astype(BF16)

    def run(index, low, blocks):
        rows = pl.ds(pl.multiple_of(index * block, block), block)
        seg_q = segc_ref[rows, :]
        places, sames, tile_at = [], [], []
        for t in range(blocks):
            j = low + t
            place = pl.ds(pl.multiple_of(j * block, block), block)
            places.append(place)
            sames.append(seg_q == segr_ref[:, place])
            tile_at.append(jnp.clip(j - index, -2, 2) + 2)
        product = do_ref[rows, :].astype(F32) * ctx32_ref[rows, :]
        logs = lse_ref[rows, :]
        outs = []
        for h in range(heads):
            lanes = slice(h * width, (h + 1) * width)
            query = qkv_ref[rows, :][:, lanes]
            grad = do_ref[rows, :][:, lanes]
            inner = jnp.sum(product[:, lanes], axis=1, keepdims=True)
            log = logs[:, h : h + 1]
            query_cot = jnp.zeros((block, width), F32)
            for t in range(blocks):
                here = qkv_ref[places[t], :]
                key_rows = here[:, heads * width + h * width : heads * width + (h + 1) * width]
                value_rows = here[:, 2 * heads * width + h * width : 2 * heads * width + (h + 1) * width]
                probs = jnp.exp(score_block(query, key_rows, tiles_ref[h, tile_at[t]], sames[t]) - log)
                prob_cot = matmul_nt(grad, value_rows)
                cot = (probs * (prob_cot - inner)).astype(BF16)
                dv_ref[h, places[t], :] += matmul_tn(probs.astype(BF16), grad)
                dk_ref[h, places[t], :] += matmul_tn(cot, query)
                query_cot += matmul(cot, key_rows)
                sums_ref[h, tile_at[t]] += cot.astype(F32)
            outs.append(query_cot)
        cots_ref[rows, : heads * width] = jnp.concatenate(outs, axis=1).astype(BF16)

    @pl.loop(0, count)
    def _(index):
        low, many = key_window(seg_smem, index, block, count)
        for blocks in range(1, count + 1):
            pl.when(many == blocks)(functools.partial(run, index, low, blocks))

    both = [dk_ref[h] for h in range(heads)] + [dv_ref[h] for h in range(heads)]
    cots_ref[:, heads * width :] = jnp.concatenate(both, axis=1).astype(BF16)
    lines = []
    for h in range(heads):
        for t in range(kinds):
            if t in (0, kinds - 1):
                line = jnp.sum(sums_ref[h, t], axis=0, keepdims=True)
                lines.append(jnp.concatenate([line, jnp.zeros_like(line)], axis=1))
                continue

            def shifted(group, total):
                eight = sums_ref[h, t, pl.ds(pl.multiple_of(group * 8, 8), 8), :]
                wide = jnp.concatenate([eight, jnp.zeros_like(eight)], axis=1)
                return total + pltpu.roll(wide, lax.rem(2 * block - 8 * group, 2 * block), 1)

            total = lax.fori_loop(0, block // 8, shifted, jnp.zeros((8, 2 * block), F32))
            place = lax.broadcasted_iota(jnp.int32, total.shape, 0)
            for bit in (1, 2, 4):
                total = jnp.where((place // bit) % 2 == 1, pltpu.roll(total, 2 * block - bit, 1), total)
            lines.append(jnp.sum(total, axis=0, keepdims=True))
    total = jnp.zeros(table_ref.shape, F32)
    for t in range(kinds):
        line = jnp.concatenate([lines[h * kinds + t] for h in range(heads)] + [jnp.zeros((8 - heads, 2 * block), F32)], axis=0)
        total += lax.dot_general(
            line, buckets_ref[t], (((1,), (0,)), ((), ())), precision=lax.Precision.HIGHEST, preferred_element_type=F32
        )
    table_ref[...] = total


def attend_back(qkv, segments, tiles, ctx32, lse, mixed, wmix, buckets):
    length, width = qkv.shape
    heads, _, block, _ = tiles.shape
    size = width // (3 * heads)
    return pl.pallas_call(
        attend_back_kernel,
        name="attend_back",
        out_shape=(
            jax.ShapeDtypeStruct((length, width), BF16),
            jax.ShapeDtypeStruct((8, 128), F32),
        ),
        in_specs=[pl.BlockSpec(memory_space=pltpu.SMEM)] + [VMEM_SPEC] * 9,
        out_specs=(VMEM_SPEC,) * 2,
        scratch_shapes=[
            pltpu.VMEM((length, width // 3), BF16),
            pltpu.VMEM((heads, length, size), F32),
            pltpu.VMEM((heads, length, size), F32),
            pltpu.VMEM((heads, 5, block, block), F32),
        ],
    )(segments, qkv, segments, segments.reshape(length, 1), tiles, ctx32, lse, mixed, wmix, buckets)


def block_rows(place, owner, size):
    return pl.ds(pl.multiple_of(owner * size, size), size)


def gain_lanes(n, shape):
    row = lax.broadcasted_iota(jnp.int32, shape, 0)
    lane = lax.broadcasted_iota(jnp.int32, shape, 1)
    count = shape[1] // (4 * n)
    shift = (row // 8) * count
    inside = (lane >= shift) & (lane < shift + count)
    return inside, row - 8 * (row // 8)


def enter_kernel(
    n, x_ref, cot_ref, gain_ref, spread_ref, w_ref, wgate_ref, line_ref,
    normed_out, cot_out, wgate_out, qkv_ref, wqkv_ref, wmix_ref, gains_ref, tiles_ref,
    wfull, gfull, nfull, cfull, g4, g32,
    ring_send, ring_recv, gate_send, gate_recv, pair_send, pair_recv, cot_send, cot_recv,
    g_send, g_recv, h_send, h_recv, local_sem,
):
    place = Place(n)
    size = x_ref.shape[0]
    own_w = pltpu.make_async_copy(w_ref, wfull.at[place.d], local_sem.at[0])
    own_g = pltpu.make_async_copy(gain_ref, g4.at[place.m], local_sem.at[1])
    own_gate = pltpu.make_async_copy(wgate_ref, gfull.at[place.d], local_sem.at[2])
    for copy in (own_w, own_g, own_gate):
        copy.start()
    place.barrier(everyone=True)
    ring = RingGather(place, wfull, ring_send, ring_recv)
    gate_ring = RingGather(place, gfull, gate_send, gate_recv)
    small = [
        remote(gain_ref, g4.at[place.m], g_send.at[k], g_recv.at[k], {"mp": lax.rem(place.m + k, 4)})
        for k in range(1, 4)
    ]
    for copy in small:
        copy.start()
    own_w.wait()
    own_gate.wait()
    for way in (0, 1):
        ring.advance(way, 0)
    scale = norm_scale(x_ref[...])
    rows = block_rows(place, place.m, size)
    cfull[rows, :] = cot_ref[...].astype(BF16)
    own_g.wait()
    for k in range(1, 4):
        slot = g4.at[lax.rem(place.m + 4 - k, 4)]
        remote(slot, slot, g_send.at[k], g_recv.at[k], {"mp": place.mate}).wait_recv()
    around = [
        remote(g4, g32.at[place.d], h_send.at[k], h_recv.at[k], {"dp": lax.rem(place.d + k, n)})
        for k in range(1, n)
    ]
    for copy in around:
        copy.start()
    own_h = pltpu.make_async_copy(g4, g32.at[place.d], local_sem.at[1])
    own_h.start()
    for way in (0, 1):
        gate_ring.advance(way, 0)
    own_h.wait()
    for k in range(1, n):
        slot = g32.at[lax.rem(place.d + n - k, n)]
        remote(g4, slot, h_send.at[k], h_recv.at[k], {"dp": place.right}).wait_recv()
    pieces = g32[...].reshape(-1, 128).astype(BF16)
    wide = matmul(pieces, spread_ref[...])
    inside, kind = gain_lanes(n, wide.shape)
    gain = jnp.sum(jnp.where(inside & (kind == 0), wide, 0.0), axis=0, keepdims=True)
    gain_two = jnp.sum(jnp.where(inside & (kind == 1), wide, 0.0), axis=0, keepdims=True)
    gains_ref[...] = jnp.concatenate([gain, gain_two] + [jnp.zeros_like(gain)] * 6, axis=0)
    nfull[rows, :] = (x_ref[...] * scale * gain).astype(BF16)
    pair = PairGather(place, nfull, pair_send, pair_recv)
    cots = PairGather(place, cfull, cot_send, cot_recv)
    for chunk in range(2):
        pair.begin(chunk)
    for chunk in range(2):
        cots.begin(chunk)
    bias_tiles(line_ref, tiles_ref)
    for step in (1, 2):
        for way in (0, 1):
            ring.advance(way, step)
        if step == 1:
            pair.relay(0)
        for way in (0, 1):
            gate_ring.advance(way, step)
    pair.relay(1)
    for way in (0, 1):
        ring.advance(way, 3)
    for chunk in range(2):
        pair.end(chunk)
    out_n = pltpu.make_async_copy(nfull, normed_out, local_sem.at[2])
    out_n.start()
    for step in range(4, n // 2 + 1):
        for way in (0, 1):
            ring.advance(way, step)
    for way in (0, 1):
        gate_ring.advance(way, 3)
    cots.relay(0)
    width = qkv_ref.shape[1]
    wqkv_ref[...] = wfull[:, :, :width]
    wmix_ref[...] = wfull[:, :, width:]
    weight = wqkv_ref[...].reshape(-1, width)

    @pl.loop(0, 4)
    def _(block):
        rows = pl.ds(pl.multiple_of(block * size, size), size)
        qkv_ref[rows, :] = matmul(nfull[rows, :], weight).astype(BF16)

    cots.relay(1)
    for step in range(4, n // 2 + 1):
        for way in (0, 1):
            gate_ring.advance(way, step)
    out_g = pltpu.make_async_copy(gfull, wgate_out, local_sem.at[0])
    out_g.start()
    for chunk in range(2):
        cots.end(chunk)
    out_c = pltpu.make_async_copy(cfull, cot_out, local_sem.at[1])
    out_c.start()
    ring.finish()
    gate_ring.finish()
    for copy in small + around:
        copy.wait_send()
    out_n.wait()
    out_g.wait()
    out_c.wait()


def enter(n, x, cot, gain, spread, weights, wgate, lines, kinds=5):
    size, features = x.shape
    rows, columns = weights.shape
    wide = wgate.shape[1]
    heads = columns // 4
    count = (lines.shape[0] - 1) // kinds
    block = lines.shape[1] // 2
    return pl.pallas_call(
        functools.partial(enter_kernel, n),
        name="enter",
        out_shape=(
            jax.ShapeDtypeStruct((4 * size, features), BF16),
            jax.ShapeDtypeStruct((4 * size, features), BF16),
            jax.ShapeDtypeStruct((n, rows, wide), BF16),
            jax.ShapeDtypeStruct((4 * size, 3 * heads), BF16),
            jax.ShapeDtypeStruct((n, rows, 3 * heads), BF16),
            jax.ShapeDtypeStruct((n, rows, heads), BF16),
            jax.ShapeDtypeStruct((8, features), F32),
            jax.ShapeDtypeStruct((count, kinds, block, block), F32),
        ),
        in_specs=[VMEM_SPEC] * 7,
        out_specs=(ANY_SPEC,) * 3 + (VMEM_SPEC,) * 5,
        scratch_shapes=[
            pltpu.VMEM((n, rows, columns), BF16),
            pltpu.VMEM((n, rows, wide), BF16),
            pltpu.VMEM((4 * size, features), BF16),
            pltpu.VMEM((4 * size, features), BF16),
            pltpu.VMEM((4, 8, 128), F32),
            pltpu.VMEM((n, 4, 8, 128), F32),
            DMA((2, n // 2)), DMA((2, n // 2)),
            DMA((2, n // 2)), DMA((2, n // 2)),
            DMA((3, 2)), DMA((3, 2)),
            DMA((3, 2)), DMA((3, 2)),
            DMA((4,)), DMA((4,)),
            DMA((n,)), DMA((n,)),
            DMA((3,)),
        ],
        compiler_params=pltpu.CompilerParams(collective_id=0, has_side_effects=True),
    )(x, cot, gain, spread, weights, wgate, lines)


def middle_kernel(
    n, ctx_ref, wmix_ref, x_ref, gains_ref, wlift_ref, wdown_ref, wgate_any,
    second_out, lift_out, down_out, bend_out, slope_out, hidden_out, middle_ref,
    lfull, dfull, gate_v, sfull, own_v, bend_v, slope_v, hidden_v,
    give, got, over, came, sc_send, sc_recv,
    pair_send, pair_recv, lift_send, lift_recv, down_send, down_recv, local_sem, out_sem,
):
    place = Place(n)
    size = x_ref.shape[0]
    own_l = pltpu.make_async_copy(wlift_ref, lfull.at[place.d], local_sem.at[0])
    own_d = pltpu.make_async_copy(wdown_ref, dfull.at[place.d], local_sem.at[1])
    load_g = pltpu.make_async_copy(wgate_any, gate_v, local_sem.at[2])
    for copy in (own_l, own_d, load_g):
        copy.start()
    place.barrier()
    lift = RingGather(place, lfull, lift_send, lift_recv)
    down = RingGather(place, dfull, down_send, down_recv)
    scatter = PairScatter(place, give, got, over, came, sc_send, sc_recv)
    pair = PairGather(place, sfull, pair_send, pair_recv)
    own_l.wait()
    own_d.wait()

    def both(ring, step):
        for way in (0, 1):
            ring.advance(way, step)

    both(lift, 0)
    weight = wmix_ref[...].reshape(-1, wmix_ref.shape[2])

    def part(owner):
        return matmul_nt(ctx_ref[block_rows(place, owner, size), :], weight)

    scatter.far(part(place.far))
    scatter.twin(part(place.twin))
    scatter.mate(part(place.mate))
    own_v[...] = part(place.m)
    both(down, 0)
    both(lift, 1)
    gain = gains_ref[1:2, :]
    chunk_rows = size // 2
    for chunk in range(2):
        rows = slice(chunk * chunk_rows, (chunk + 1) * chunk_rows)
        middle = x_ref[rows, :] + scatter.take(chunk, own_v[rows, :])
        middle_ref[rows, :] = middle
        start = pl.multiple_of(place.m * size + chunk * chunk_rows, chunk_rows)
        sfull[pl.ds(start, chunk_rows), :] = (middle * norm_scale(middle) * gain).astype(BF16)
        pair.begin(chunk)
    load_g.wait()

    def gate_block(owner):
        rows = block_rows(place, owner, size)
        gate = matmul(sfull[rows, :], gate_v[...].reshape(-1, gate_v.shape[2]))
        bend, slope = gate_terms(gate)
        bend_v[rows, :] = bend
        slope_v[rows, :] = slope

    gate_block(place.m)
    both(down, 1)
    both(lift, 2)
    pair.relay(0)
    pair.relay(1)
    both(down, 2)
    both(lift, 3)
    for chunk in range(2):
        pair.end(chunk)
    out_s = pltpu.make_async_copy(sfull, second_out, local_sem.at[0])
    out_s.start()

    @pl.loop(1, 4)
    def _(k):
        gate_block(lax.rem(place.m + k, 4))

    both(lift, 4)
    out_b = pltpu.make_async_copy(bend_v, bend_out, local_sem.at[1])
    out_b.start()
    out_l = pltpu.make_async_copy(lfull, lift_out, local_sem.at[2])
    out_l.start()
    both(down, 3)

    @pl.loop(0, 4)
    def _(k):
        rows = pl.ds(pl.multiple_of(k * size, size), size)
        lifted = matmul(sfull[rows, :], lfull[...].reshape(-1, lfull.shape[2]))
        hidden_v[rows, :] = (bend_v[rows, :] * lifted).astype(BF16)
        slope_v[rows, :] = slope_v[rows, :] * lifted

    out_p = pltpu.make_async_copy(slope_v, slope_out, out_sem.at[0])
    out_h = pltpu.make_async_copy(hidden_v, hidden_out, out_sem.at[1])
    out_d = pltpu.make_async_copy(dfull, down_out, out_sem.at[2])
    out_p.start()
    out_h.start()
    both(down, 4)
    out_d.start()
    lift.finish()
    down.finish()
    scatter.finish()
    for copy in (out_s, out_b, out_l, out_p, out_h, out_d):
        copy.wait()


def middle_part(n, ctx, wmix, x, gains, wlift, wdown, wgate):
    size, features = x.shape
    rows, wide = wlift.shape
    length = 4 * size
    full = jax.ShapeDtypeStruct((n, rows, wide), BF16)
    return pl.pallas_call(
        functools.partial(middle_kernel, n),
        name="middle",
        out_shape=(
            jax.ShapeDtypeStruct((length, features), BF16),
            full,
            full,
            jax.ShapeDtypeStruct((length, wide), F32),
            jax.ShapeDtypeStruct((length, wide), F32),
            jax.ShapeDtypeStruct((length, wide), BF16),
            jax.ShapeDtypeStruct((size, features), F32),
        ),
        in_specs=[VMEM_SPEC] * 6 + [ANY_SPEC],
        out_specs=(ANY_SPEC,) * 6 + (VMEM_SPEC,),
        scratch_shapes=[
            pltpu.VMEM((n, rows, wide), BF16),
            pltpu.VMEM((n, rows, wide), BF16),
            pltpu.VMEM((n, rows, wide), BF16),
            pltpu.VMEM((length, features), BF16),
            pltpu.VMEM((size, features), F32),
            pltpu.VMEM((length, wide), F32),
            pltpu.VMEM((length, wide), F32),
            pltpu.VMEM((length, wide), BF16),
            *PairScatter.scratch(size, features),
            DMA((3, 2)), DMA((3, 2)),
            DMA((2, n // 2)), DMA((2, n // 2)),
            DMA((2, n // 2)), DMA((2, n // 2)),
            DMA((3,)), DMA((3,)),
        ],
        compiler_params=pltpu.CompilerParams(collective_id=1, has_side_effects=True),
    )(ctx, wmix, x, gains, wlift, wdown, wgate)


def norm_back(values, gain, grad):
    scale = norm_scale(values)
    term = grad * values
    inner = jnp.mean(term * gain, axis=-1, keepdims=True)
    return gain * scale * grad - values * (scale * scale * scale * inner), term * scale


def back_kernel(
    n, middle_ref, cotangent_ref, gains_ref, hidden_any, cot_any, second_any, bend_any, slope_any, wgate_any, wlift_any, wdown_any,
    mixed_out, middle_cot_ref, feed_ref, grad_down_ref, grad_gate_ref, grad_lift_ref,
    hidden_v, cot_v, second_v, gate_v, lift_v, down_v, bend_v, slope_v, gcot_v, lcot_v, mixed_v, own_v,
    give, got, over, came, sc_send, sc_recv,
    pair_send, pair_recv,
    put_d, in_d, send_d, recv_d, put_g, in_g, send_g, recv_g, put_l, in_l, send_l, recv_l,
    load_sem, piece_sem, out_sem,
):
    place = Place(n)
    size = middle_ref.shape[0]
    loads = [
        pltpu.make_async_copy(source, target, load_sem.at[k])
        for k, (source, target) in enumerate(
            ((hidden_any, hidden_v), (cot_any, cot_v), (wdown_any, down_v), (wgate_any, gate_v), (wlift_any, lift_v), (second_any, second_v))
        )
    ]
    for copy in loads:
        copy.start()
    order = (place.far, place.twin, place.mate, place.m)

    def pieces(k):
        rows = block_rows(place, order[k], size)
        return [
            pltpu.make_async_copy(source.at[rows], target.at[k % 2], piece_sem.at[k % 2, i])
            for i, (source, target) in enumerate(((bend_any, bend_v), (slope_any, slope_v)))
        ]

    for copy in pieces(0):
        copy.start()
    place.barrier()
    down = RingScatter(place, lambda slot: matmul_tn(slot_columns(cot_v, slot, n), hidden_v[...]), grad_down_ref, put_d, in_d, send_d, recv_d)
    gate = RingScatter(place, lambda slot: matmul_tn(slot_columns(second_v, slot, n), gcot_v[...]), grad_gate_ref, put_g, in_g, send_g, recv_g)
    lift = RingScatter(place, lambda slot: matmul_tn(slot_columns(second_v, slot, n), lcot_v[...]), grad_lift_ref, put_l, in_l, send_l, recv_l)
    scatter = PairScatter(place, give, got, over, came, sc_send, sc_recv)
    pair = PairGather(place, mixed_v, pair_send, pair_recv)

    def both(ring, step):
        for way in (0, 1):
            ring.advance(way, step)

    def flat(ref):
        return ref[...].reshape(-1, ref.shape[2])

    loads[0].wait()
    loads[1].wait()
    both(down, 0)
    for copy in loads[2:5]:
        copy.wait()
    for k in range(4):
        rows = block_rows(place, order[k], size)
        if k < 3:
            for copy in pieces(k + 1):
                copy.start()
        hidden_cot = matmul(cot_v[rows, :], flat(down_v))
        for copy in pieces(k):
            copy.wait()
        gate_cot = (hidden_cot * slope_v[k % 2]).astype(BF16)
        lift_cot = (hidden_cot * bend_v[k % 2]).astype(BF16)
        gcot_v[rows, :] = gate_cot
        lcot_v[rows, :] = lift_cot
        part = matmul_nt(gate_cot, flat(gate_v)) + matmul_nt(lift_cot, flat(lift_v))
        if k == 0:
            scatter.far(part)
        elif k == 1:
            scatter.twin(part)
            both(down, 1)
        elif k == 2:
            scatter.mate(part)
        else:
            own_v[...] = part
    loads[5].wait()
    both(gate, 0)
    both(down, 2)
    both(lift, 0)
    chunk_rows = size // 2
    gain = gains_ref[1:2, :]
    feed = jnp.zeros_like(gain)
    for chunk in range(2):
        rows = slice(chunk * chunk_rows, (chunk + 1) * chunk_rows)
        grad = scatter.take(chunk, own_v[rows, :])
        through, term = norm_back(middle_ref[rows, :], gain, grad)
        middle_cot = cotangent_ref[rows, :] + through
        middle_cot_ref[rows, :] = middle_cot
        feed += jnp.sum(term, axis=0, keepdims=True)
        start = pl.multiple_of(place.m * size + chunk * chunk_rows, chunk_rows)
        mixed_v[pl.ds(start, chunk_rows), :] = middle_cot.astype(BF16)
        pair.begin(chunk)
    feed_ref[...] = jnp.concatenate([feed] + [jnp.zeros_like(feed)] * 7, axis=0)
    scatter.finish()
    both(gate, 1)
    both(down, 3)
    both(lift, 1)
    pair.relay(0)
    pair.relay(1)
    both(gate, 2)
    down.finish()
    both(lift, 2)
    for chunk in range(2):
        pair.end(chunk)
    out_m = pltpu.make_async_copy(mixed_v, mixed_out, out_sem.at[0])
    out_m.start()
    both(gate, 3)
    both(lift, 3)
    gate.finish()
    lift.finish()
    out_m.wait()


def back_part(n, middle, cotangent, gains, hidden, cot, second, bend, slope, wgate, wlift, wdown):
    size, features = middle.shape
    length, wide = hidden.shape
    rows = wgate.shape[1]
    grad = jax.ShapeDtypeStruct((rows, wide), F32)
    weight = pltpu.VMEM((n, rows, wide), BF16)
    return pl.pallas_call(
        functools.partial(back_kernel, n),
        name="back",
        out_shape=(
            jax.ShapeDtypeStruct((length, features), BF16),
            jax.ShapeDtypeStruct((size, features), F32),
            jax.ShapeDtypeStruct((8, features), F32),
            grad, grad, grad,
        ),
        in_specs=[VMEM_SPEC] * 3 + [ANY_SPEC] * 8,
        out_specs=(ANY_SPEC,) + (VMEM_SPEC,) * 5,
        scratch_shapes=[
            pltpu.VMEM((length, wide), BF16),
            pltpu.VMEM((length, features), BF16),
            pltpu.VMEM((length, features), BF16),
            weight, weight, weight,
            pltpu.VMEM((2, size, wide), F32),
            pltpu.VMEM((2, size, wide), F32),
            pltpu.VMEM((length, wide), BF16),
            pltpu.VMEM((length, wide), BF16),
            pltpu.VMEM((length, features), BF16),
            pltpu.VMEM((size, features), F32),
            *PairScatter.scratch(size, features),
            DMA((3, 2)), DMA((3, 2)),
            *RingScatter.scratch(n, rows, wide),
            *RingScatter.scratch(n, rows, wide),
            *RingScatter.scratch(n, rows, wide),
            DMA((6,)), DMA((2, 2)), DMA((1,)),
        ],
        compiler_params=pltpu.CompilerParams(collective_id=2, has_side_effects=True, vmem_limit_bytes=67043328),
    )(middle, cotangent, gains, hidden, cot, second, bend, slope, wgate, wlift, wdown)


def leave_kernel(
    n, cots_ref, ctx_ref, wqkv_ref, x_ref, gains_ref, middle_cot_ref, feed_ref, table_ref, spread_ref,
    middle_ref, hidden_ref, normed_any, mixed_any, wdown_any,
    grad_ref, gain_out, table_out, input_ref, output_ref,
    normed_v, mixed_v, down_v, own_v, own_two,
    give, got, over, came, sc_send, sc_recv,
    give_two, got_two, over_two, came_two, sd_send, sd_recv,
    put, inbox, ring_send, ring_recv,
    tables, pieces_v, spare_v, sum_v, last_v,
    t_send, t_recv, g_send, g_recv, h_send, h_recv, load_sem,
):
    place = Place(n)
    size = x_ref.shape[0]
    load_n = pltpu.make_async_copy(normed_any, normed_v, load_sem.at[0])
    load_m = pltpu.make_async_copy(mixed_any, mixed_v, load_sem.at[1])
    load_d = pltpu.make_async_copy(wdown_any, down_v, load_sem.at[2])
    for copy in (load_n, load_m, load_d):
        copy.start()
    place.barrier(everyone=True)

    def peer(k):
        return {"dp": lax.rem(place.d + k, n)}

    table_copies = [remote(table_ref, tables.at[n - k], t_send.at[k], t_recv.at[k], peer(k)) for k in range(1, n)]
    for copy in table_copies:
        copy.start()
    scatter = PairScatter(place, give, got, over, came, sc_send, sc_recv)
    downs = PairScatter(place, give_two, got_two, over_two, came_two, sd_send, sd_recv)

    def term(slot):
        left = matmul_tn(slot_columns(normed_v, slot, n), cots_ref[...])
        return jnp.concatenate([left, matmul_tn(slot_columns(mixed_v, slot, n), ctx_ref[...])], axis=1)

    ring = RingScatter(place, term, grad_ref, put, inbox, ring_send, ring_recv)

    def both(step):
        for way in (0, 1):
            ring.advance(way, step)

    def part(owner):
        weight = wqkv_ref[...].reshape(-1, wqkv_ref.shape[2])
        return matmul_nt(cots_ref[block_rows(place, owner, size), :], weight)

    def part_two(owner):
        weight = down_v[...].reshape(-1, down_v.shape[2])
        return matmul_nt(hidden_ref[block_rows(place, owner, size), :], weight)

    scatter.far(part(place.far))
    scatter.twin(part(place.twin))
    load_n.wait()
    load_m.wait()
    both(0)
    scatter.mate(part(place.mate))
    own_v[...] = part(place.m)
    load_d.wait()
    downs.far(part_two(place.far))
    downs.twin(part_two(place.twin))
    both(1)
    downs.mate(part_two(place.mate))
    own_two[...] = part_two(place.m)
    both(2)
    chunk_rows = size // 2
    gain = gains_ref[0:1, :]
    total = jnp.zeros_like(gain)
    for chunk in range(2):
        rows = slice(chunk * chunk_rows, (chunk + 1) * chunk_rows)
        grad = scatter.take(chunk, own_v[rows, :])
        through, terms = norm_back(x_ref[rows, :], gain, grad)
        input_ref[rows, :] = middle_cot_ref[rows, :] + through
        total += jnp.sum(terms, axis=0, keepdims=True)
    inside, kind = gain_lanes(n, (n * 4 * 8, gain.shape[1]))
    rows = jnp.where(inside & (kind == 0), total, 0.0) + jnp.where(inside & (kind == 1), feed_ref[0:1, :], 0.0)
    rows = lax.dot_general(
        rows, spread_ref[...].astype(F32), (((1,), (1,)), ((), ())), precision=lax.Precision.HIGHEST, preferred_element_type=F32
    )
    pieces_v[...] = rows.reshape(pieces_v.shape)
    around = [remote(pieces_v.at[lax.rem(place.d + k, n)], spare_v.at[n - k], g_send.at[k], g_recv.at[k], peer(k)) for k in range(1, n)]
    for copy in around:
        copy.start()
    both(3)
    table = table_ref[...]
    for k in range(1, n):
        remote(table_ref, tables.at[n - k], t_send.at[k], t_recv.at[k], peer(k)).wait_recv()
        table += tables[n - k]
    table_out[...] = table
    sums = pieces_v[place.d]
    for k in range(1, n):
        remote(pieces_v.at[0], spare_v.at[n - k], g_send.at[k], g_recv.at[k], peer(k)).wait_recv()
        sums += spare_v[n - k]
    sum_v[...] = sums
    last = []
    for k in range(1, 4):
        target = lax.rem(place.m + k, 4)
        last.append(remote(sum_v.at[target], last_v.at[4 - k], h_send.at[k], h_recv.at[k], {"mp": target}))
        last[-1].start()
    for chunk in range(2):
        rows = slice(chunk * chunk_rows, (chunk + 1) * chunk_rows)
        output_ref[rows, :] = middle_ref[rows, :] + downs.take(chunk, own_two[rows, :])
    ring.finish()
    sums = sum_v[place.m]
    for k in range(1, 4):
        remote(sum_v.at[0], last_v.at[4 - k], h_send.at[k], h_recv.at[k], {"mp": place.mate}).wait_recv()
        sums += last_v[4 - k]
    gain_out[...] = sums
    scatter.finish()
    downs.finish()
    for copy in table_copies + around + last:
        copy.wait_send()


def leave_part(n, cots, ctx, wqkv, x, gains, middle_cot, feed, table, spread, middle, hidden, normed, mixed, wdown):
    size, features = x.shape
    length, width = cots.shape
    rows = wqkv.shape[1]
    columns = width + ctx.shape[1]
    return pl.pallas_call(
        functools.partial(leave_kernel, n),
        name="leave",
        out_shape=(
            jax.ShapeDtypeStruct((rows, columns), F32),
            jax.ShapeDtypeStruct((8, 128), F32),
            jax.ShapeDtypeStruct((8, 128), F32),
            jax.ShapeDtypeStruct((size, features), F32),
            jax.ShapeDtypeStruct((size, features), F32),
        ),
        in_specs=[VMEM_SPEC] * 11 + [ANY_SPEC] * 3,
        out_specs=(VMEM_SPEC,) * 5,
        scratch_shapes=[
            pltpu.VMEM((length, features), BF16),
            pltpu.VMEM((length, features), BF16),
            pltpu.VMEM(wdown.shape, BF16),
            pltpu.VMEM((size, features), F32),
            pltpu.VMEM((size, features), F32),
            *PairScatter.scratch(size, features),
            *PairScatter.scratch(size, features),
            *RingScatter.scratch(n, rows, columns),
            pltpu.VMEM((n, 8, 128), F32),
            pltpu.VMEM((n, 4, 8, 128), F32),
            pltpu.VMEM((n, 4, 8, 128), F32),
            pltpu.VMEM((4, 8, 128), F32),
            pltpu.VMEM((4, 8, 128), F32),
            DMA((n,)), DMA((n,)),
            DMA((n,)), DMA((n,)),
            DMA((4,)), DMA((4,)),
            DMA((3,)),
        ],
        compiler_params=pltpu.CompilerParams(collective_id=3, has_side_effects=True),
    )(cots, ctx, wqkv, x, gains, middle_cot, feed, table, spread, middle, hidden, normed, mixed, wdown)


THRESHOLDS = (8, 12, 16, 23, 32, 46, 64, 91)
HIGHEST = lax.Precision.HIGHEST
MASKED = -1e30


def bucket_table(length):
    places = jnp.arange(length, dtype=jnp.int32)
    offset = places[None, :] - places[:, None]
    distance = jnp.abs(offset)
    far_bucket = 7 + sum(((distance >= limit).astype(jnp.int32) for limit in THRESHOLDS))
    near = jnp.where(distance < 8, distance, far_bucket)
    return near + jnp.where(offset > 0, 16, 0).astype(jnp.int32)


def scaled_norm(values, gain):
    return values * lax.rsqrt(jnp.mean(values * values, axis=-1, keepdims=True) + EPSILON) * gain


def gated(gate, lift):
    return jax.nn.gelu(gate, approximate=True) * lift


def dense(left, weight):
    return jnp.einsum("rld,de->rle", left, weight, preferred_element_type=jnp.float32)


def dense_back(grad, weight):
    return jnp.einsum("rle,de->rld", grad, weight, preferred_element_type=jnp.float32)


def weight_term(left, grad):
    return jnp.einsum("rld,rle->de", left, grad, preferred_element_type=jnp.float32)


def collect(part):
    return lax.all_gather(part, "mp", axis=1, tiled=True)


def spread(part):
    return lax.psum_scatter(part, "mp", scatter_dimension=1, tiled=True)


def split_heads(rows, count):
    return rows.reshape(rows.shape[0], count, rows.shape[1] // count)


def bias_blocks(table_part, buckets):
    length = buckets.shape[0]
    block = min(length, 128)
    tiles = buckets.reshape(length // block, block, length)
    codes = jnp.arange(table_part.shape[0], dtype=jnp.int32)

    def bias_one_block(tile):
        onehot = (tile[None] == codes[:, None, None]).astype(jnp.float32)
        return jnp.einsum("bij,bh->hij", onehot, table_part, precision=HIGHEST)

    pieces = lax.map(bias_one_block, tiles)
    return jnp.transpose(pieces, (1, 0, 2, 3)).reshape(table_part.shape[1], length, length)


def table_terms(score_total, buckets, count):
    heads_here, length, _ = score_total.shape
    block = min(length, 128)
    tiles = buckets.reshape(length // block, block, length)
    pieces = jnp.transpose(
        score_total.reshape(heads_here, length // block, block, length), (1, 0, 2, 3)
    )
    codes = jnp.arange(count, dtype=jnp.int32)

    def table_one_block(total, pair):
        tile, piece = pair
        onehot = (tile[None] == codes[:, None, None]).astype(jnp.float32)
        return (total + jnp.einsum("bij,hij->bh", onehot, piece, precision=HIGHEST), None)

    result, _ = lax.scan(
        table_one_block, jnp.zeros((count, heads_here), jnp.float32), (tiles, pieces)
    )
    return result


def native(
    inputs,
    segments,
    attend_gain,
    feed_gain,
    w_query,
    w_key,
    w_value,
    w_mixer,
    rel_table,
    w_gate,
    w_lift,
    w_down,
    cotangent,
):
    length = segments.shape[1]
    heads_here = rel_table.shape[1]
    buckets = bucket_table(length)
    bias = bias_blocks(rel_table, buckets)
    gains = (
        lax.all_gather(attend_gain.astype(jnp.bfloat16), ("dp", "mp"), axis=0, tiled=True),
        lax.all_gather(feed_gain.astype(jnp.bfloat16), ("dp", "mp"), axis=0, tiled=True),
    )
    first_gain = gains[0].astype(jnp.float32)
    second_gain = gains[1].astype(jnp.float32)
    attention_full = (
        lax.all_gather(w_query.astype(jnp.bfloat16), "dp", axis=0, tiled=True),
        lax.all_gather(w_key.astype(jnp.bfloat16), "dp", axis=0, tiled=True),
        lax.all_gather(w_value.astype(jnp.bfloat16), "dp", axis=0, tiled=True),
        lax.all_gather(w_mixer.astype(jnp.bfloat16), "dp", axis=1, tiled=True),
    )
    feed_full = (
        lax.all_gather(w_gate.astype(jnp.bfloat16), "dp", axis=0, tiled=True),
        lax.all_gather(w_lift.astype(jnp.bfloat16), "dp", axis=0, tiled=True),
        lax.all_gather(w_down.astype(jnp.bfloat16), "dp", axis=1, tiled=True),
    )

    def score_rows(query_heads, key_heads, segment_row):
        scores = (
            jnp.einsum("ihe,jhe->hij", query_heads, key_heads, preferred_element_type=jnp.float32)
            + bias
        )
        same = segment_row[:, None] == segment_row[None, :]
        return jnp.where(same[None], scores, MASKED)

    normed = scaled_norm(inputs, first_gain).astype(jnp.bfloat16)
    normed_full = collect(normed)
    query = dense(normed_full, attention_full[0]).astype(jnp.bfloat16)
    keys = dense(normed_full, attention_full[1]).astype(jnp.bfloat16)
    values = dense(normed_full, attention_full[2]).astype(jnp.bfloat16)

    def attend(row):
        query_row, key_row, value_row, segment_row = row
        query_heads = split_heads(query_row, heads_here)
        key_heads = split_heads(key_row, heads_here)
        value_heads = split_heads(value_row, heads_here)
        scores = score_rows(query_heads, key_heads, segment_row)
        largest = jnp.max(scores, axis=-1, keepdims=True)
        raised = jnp.exp(scores - largest)
        totals = jnp.sum(raised, axis=-1, keepdims=True)
        probs = (raised / totals).astype(jnp.bfloat16)
        context = jnp.einsum("hij,jhe->ihe", probs, value_heads, preferred_element_type=jnp.float32)
        return (
            context.astype(jnp.bfloat16).reshape(length, -1),
            (largest + jnp.log(totals))[..., 0],
        )

    context, logsum = lax.map(attend, (query, keys, values, segments))
    middle = inputs + spread(dense(context, attention_full[3]))
    normed_two = scaled_norm(middle, second_gain).astype(jnp.bfloat16)
    second_full = collect(normed_two)
    gate = dense(second_full, feed_full[0])
    lift = dense(second_full, feed_full[1])
    hidden = gated(gate, lift).astype(jnp.bfloat16)
    output = middle + spread(dense(hidden, feed_full[2]))
    feed_back = (
        lax.all_gather(w_gate.astype(jnp.bfloat16), "dp", axis=0, tiled=True),
        lax.all_gather(w_lift.astype(jnp.bfloat16), "dp", axis=0, tiled=True),
        lax.all_gather(w_down.astype(jnp.bfloat16), "dp", axis=1, tiled=True),
    )
    down_full = collect(cotangent.astype(jnp.bfloat16))
    hidden_cot = dense_back(down_full, feed_back[2])
    down_term = weight_term(hidden, down_full)
    _, gated_pull = jax.vjp(gated, gate, lift)
    gate_cot, lift_cot = gated_pull(hidden_cot)
    gate_cot = gate_cot.astype(jnp.bfloat16)
    lift_cot = lift_cot.astype(jnp.bfloat16)
    gate_term = weight_term(second_full, gate_cot)
    lift_term = weight_term(second_full, lift_cot)
    second_cot = spread(dense_back(gate_cot, feed_back[0]) + dense_back(lift_cot, feed_back[1]))
    _, second_pull = jax.vjp(scaled_norm, middle, second_gain)
    middle_from_norm, second_gain_term = second_pull(second_cot)
    middle_cot = cotangent + middle_from_norm
    attention_back = (
        lax.all_gather(w_query.astype(jnp.bfloat16), "dp", axis=0, tiled=True),
        lax.all_gather(w_key.astype(jnp.bfloat16), "dp", axis=0, tiled=True),
        lax.all_gather(w_value.astype(jnp.bfloat16), "dp", axis=0, tiled=True),
        lax.all_gather(w_mixer.astype(jnp.bfloat16), "dp", axis=1, tiled=True),
    )
    mixed_full = collect(middle_cot.astype(jnp.bfloat16))
    context_cot = dense_back(mixed_full, attention_back[3]).astype(jnp.bfloat16)
    mixer_term = weight_term(context, mixed_full)

    def attend_back(total, row):
        query_row, key_row, value_row, segment_row, log_row, cot_row = row
        query_heads = split_heads(query_row, heads_here)
        key_heads = split_heads(key_row, heads_here)
        value_heads = split_heads(value_row, heads_here)
        cot_heads = split_heads(cot_row, heads_here)
        scores = score_rows(query_heads, key_heads, segment_row)
        probs = jnp.exp(scores - log_row[:, :, None])
        value_cot = jnp.einsum(
            "hij,ihe->jhe",
            probs.astype(jnp.bfloat16),
            cot_heads,
            preferred_element_type=jnp.float32,
        )
        prob_cot = jnp.einsum(
            "ihe,jhe->hij", cot_heads, value_heads, preferred_element_type=jnp.float32
        )
        inner = jnp.sum(probs * prob_cot, axis=-1, keepdims=True)
        score_cot = (probs * (prob_cot - inner)).astype(jnp.bfloat16)
        query_cot = jnp.einsum(
            "hij,jhe->ihe", score_cot, key_heads, preferred_element_type=jnp.float32
        )
        key_cot = jnp.einsum(
            "hij,ihe->jhe", score_cot, query_heads, preferred_element_type=jnp.float32
        )
        outputs = (
            query_cot.astype(jnp.bfloat16).reshape(length, -1),
            key_cot.astype(jnp.bfloat16).reshape(length, -1),
            value_cot.astype(jnp.bfloat16).reshape(length, -1),
        )
        return (total + score_cot.astype(jnp.float32), outputs)

    score_total, cots = lax.scan(
        attend_back,
        jnp.zeros((heads_here, length, length), jnp.float32),
        (query, keys, values, segments, logsum, context_cot),
    )
    query_cot, key_cot, value_cot = cots
    query_term = weight_term(normed_full, query_cot)
    key_term = weight_term(normed_full, key_cot)
    value_term = weight_term(normed_full, value_cot)
    first_cot = spread(
        dense_back(query_cot, attention_back[0])
        + dense_back(key_cot, attention_back[1])
        + dense_back(value_cot, attention_back[2])
    )
    _, first_pull = jax.vjp(scaled_norm, inputs, first_gain)
    input_from_norm, first_gain_term = first_pull(first_cot)
    input_grad = middle_cot + input_from_norm
    table_grad = lax.psum(table_terms(score_total, buckets, rel_table.shape[0]), "dp")
    gain_grads = (
        lax.psum_scatter(first_gain_term, ("dp", "mp"), scatter_dimension=0, tiled=True),
        lax.psum_scatter(second_gain_term, ("dp", "mp"), scatter_dimension=0, tiled=True),
    )
    summed = (
        lax.psum_scatter(query_term, "dp", scatter_dimension=0, tiled=True),
        lax.psum_scatter(key_term, "dp", scatter_dimension=0, tiled=True),
        lax.psum_scatter(value_term, "dp", scatter_dimension=0, tiled=True),
        lax.psum_scatter(mixer_term, "dp", scatter_dimension=1, tiled=True),
        lax.psum_scatter(gate_term, "dp", scatter_dimension=0, tiled=True),
        lax.psum_scatter(lift_term, "dp", scatter_dimension=0, tiled=True),
        lax.psum_scatter(down_term, "dp", scatter_dimension=1, tiled=True),
    )
    return (
        output,
        input_grad,
        gain_grads[0],
        gain_grads[1],
        summed[0],
        summed[1],
        summed[2],
        summed[3],
        table_grad,
        summed[4],
        summed[5],
        summed[6],
    )


BLOCK = 256
KINDS = 5


def tile_buckets(block):
    column = jnp.arange(2 * block)
    column = jnp.where(column < block, column, column - 2 * block)
    kind = jnp.arange(KINDS)[:, None]
    offset = column[None, :] + (kind - 2) * block
    offset = jnp.where(kind == 0, -2 * block, jnp.where(kind == KINDS - 1, 2 * block, offset))
    distance = jnp.abs(offset)
    far_bucket = 7 + sum(((distance >= limit).astype(jnp.int32) for limit in THRESHOLDS))
    return jnp.where(distance < 8, distance, far_bucket) + jnp.where(offset > 0, 16, 0)


def fused(
    n,
    inputs,
    segments,
    attend_gain,
    feed_gain,
    w_query,
    w_key,
    w_value,
    w_mixer,
    rel_table,
    w_gate,
    w_lift,
    w_down,
    cotangent,
):
    x, cot = inputs[0], cotangent[0]
    size = x.shape[0]
    hidden_here = w_gate.shape[1]
    heads = rel_table.shape[1]
    head_width = w_query.shape[1]
    per = attend_gain.shape[0]
    spare = -hidden_here % 128
    gain = jnp.pad(jnp.stack([attend_gain, feed_gain]), ((0, 6), (0, 128 - per)))
    spread_rows = (jnp.arange(x.shape[1])[None, :] % per == jnp.arange(128)[:, None]).astype(BF16)
    attention = jnp.concatenate([w_query, w_key, w_value, w_mixer.T], axis=1).astype(BF16)
    wgate, wlift, wdown = (
        jnp.pad(part.astype(BF16), ((0, 0), (0, spare))) for part in (w_gate, w_lift, w_down.T)
    )
    onehot = (tile_buckets(BLOCK)[..., None] == jnp.arange(128)).astype(F32)
    count = rel_table.shape[0]
    lines = jnp.einsum("tkb,bh->htk", onehot[..., :count], rel_table, precision=HIGHEST)
    lines = jnp.pad(lines.reshape(heads * KINDS, -1), ((0, 1), (0, 0)))

    normed, cots, gate_full, qkv, wqkv, wmix, gains, tiles = enter(
        n, x, cot, gain, spread_rows, attention, wgate, lines
    )
    context, context32, logsum = attend(qkv, segments, tiles)
    second, lift_full, down_full, bend, slope, hidden, middle = middle_part(
        n, context, wmix, x, gains, wlift, wdown, gate_full
    )
    mixed, middle_cot, feed, down_term, gate_term, lift_term = back_part(
        n, middle, cot, gains, hidden, cots, second, bend, slope, gate_full, lift_full, down_full
    )
    qkv_cot, table = attend_back(qkv, segments, tiles, context32, logsum, mixed, wmix, onehot)
    attention_term, gain_term, table_term, input_grad, output = leave_part(
        n, qkv_cot, context, wqkv, x, gains, middle_cot, feed, table, spread_rows, middle, hidden, normed, mixed, down_full
    )
    return (
        output[None],
        input_grad[None],
        gain_term[0, :per],
        gain_term[1, :per],
        attention_term[:, :head_width],
        attention_term[:, head_width : 2 * head_width],
        attention_term[:, 2 * head_width : 3 * head_width],
        attention_term[:, 3 * head_width :].T,
        table_term[:heads, :count].T,
        gate_term[:, :hidden_here],
        lift_term[:, :hidden_here],
        down_term[:, :hidden_here].T,
    )


def kernels_fit(mesh):
    return mesh.shape["dp"] == 8 and mesh.shape["mp"] == 4


def solution(mesh):
    local = functools.partial(fused, mesh.shape["dp"]) if kernels_fit(mesh) else native
    return jax.shard_map(
        local,
        mesh=mesh,
        in_specs=(
            P("dp", "mp", None),
            P("dp", None),
            P(("dp", "mp")),
            P(("dp", "mp")),
            P("dp", "mp"),
            P("dp", "mp"),
            P("dp", "mp"),
            P("mp", "dp"),
            P(None, "mp"),
            P("dp", "mp"),
            P("dp", "mp"),
            P("mp", "dp"),
            P("dp", "mp", None),
        ),
        out_specs=(
            P("dp", "mp", None),
            P("dp", "mp", None),
            P(("dp", "mp")),
            P(("dp", "mp")),
            P("dp", "mp"),
            P("dp", "mp"),
            P("dp", "mp"),
            P("mp", "dp"),
            P(None, "mp"),
            P("dp", "mp"),
            P("dp", "mp"),
            P("mp", "dp"),
        ),
        check_vma=False,
    )
```

```python
import functools

import jax
import jax.numpy as jnp
from jax import lax
from jax.experimental import pallas as pl
from jax.experimental.pallas import tpu as pltpu
from jax.sharding import PartitionSpec as P

EPSILON = 1e-06
THRESHOLDS = (8, 12, 16, 23, 32, 46, 64, 91)
HIGHEST = lax.Precision.HIGHEST
MASKED = -1e30
BLOCK = 256
KINDS = 5
MESH = pl.DeviceIdType.MESH
BF16 = jnp.bfloat16
F32 = jnp.float32
VMEM_SPEC = pl.BlockSpec(memory_space=pltpu.VMEM)
ANY_SPEC = pl.BlockSpec(memory_space=pl.ANY)
DMA = pltpu.SemaphoreType.DMA


def remote(source, target, send_sem, recv_sem, where):
    return pltpu.make_async_remote_copy(
        src_ref=source,
        dst_ref=target,
        send_sem=send_sem,
        recv_sem=recv_sem,
        device_id=where,
        device_id_type=MESH,
    )


def matmul(left, right):
    return lax.dot_general(left, right, (((1,), (0,)), ((), ())), preferred_element_type=F32)


def matmul_nt(left, right):
    return lax.dot_general(left, right, (((1,), (1,)), ((), ())), preferred_element_type=F32)


def matmul_tn(left, right):
    return lax.dot_general(left, right, (((0,), (0,)), ((), ())), preferred_element_type=F32)


class Place:
    def __init__(self, n):
        self.n = n
        self.d = lax.axis_index("dp")
        self.m = lax.axis_index("mp")
        self.pos = lax.rem(self.d, 2) * (n - 1) + (self.d // 2) * (1 - 2 * lax.rem(self.d, 2))
        self.right = self.device(self.pos + 1)
        self.left = self.device(self.pos + n - 1)
        self.mate = self.m + 1 - 2 * lax.rem(self.m, 2)
        self.twin = lax.rem(self.m + 2, 4)
        self.far = lax.rem(self.mate + 2, 4)

    def device(self, position):
        position = lax.rem(position, self.n)
        late = position // (self.n // 2)
        return 2 * position * (1 - late) + (2 * (self.n - 1 - position) + 1) * late

    def barrier(self, ring=True, pair=True, everyone=False):
        sem = pltpu.get_barrier_semaphore()
        partners = []
        if everyone:
            partners += [{"dp": lax.rem(self.d + k, self.n)} for k in range(1, self.n)]
        elif ring:
            partners += [{"dp": self.right}, {"dp": self.left}]
        if pair:
            partners += [{"mp": self.mate}, {"mp": self.twin}, {"mp": self.far}]
        for where in partners:
            pl.semaphore_signal(sem, inc=1, device_id=where, device_id_type=MESH)
        pl.semaphore_wait(sem, len(partners))


class RingGather:
    def __init__(self, place, full, send, recv, first=0):
        self.place, self.full, self.send, self.recv = place, full, send, recv
        self.steps, self.first = place.n // 2, first

    def part(self, way, position, step):
        slot = self.full.at[self.place.device(position + self.place.n)]
        if step < self.steps - 1:
            return slot
        half = self.full.shape[1] // 2
        return slot.at[pl.ds(half * way, half)]

    def outgoing(self, way, step):
        ref = self.part(way, self.place.pos + (step if way else -step), step)
        where = {"dp": self.place.left if way else self.place.right}
        return remote(ref, ref, self.send.at[way, step], self.recv.at[way, step], where)

    def incoming(self, way, step):
        ref = self.part(way, self.place.pos + (1 + step if way else -1 - step), step)
        where = {"dp": self.place.left if way else self.place.right}
        return remote(ref, ref, self.send.at[way, step], self.recv.at[way, step], where)

    def advance(self, way, step):
        if step > self.first:
            self.incoming(way, step - 1).wait_recv()
        if step < self.steps:
            self.outgoing(way, step).start()

    def finish(self):
        for way in (0, 1):
            for step in range(self.first, self.steps):
                self.outgoing(way, step).wait_send()


class PairGather:
    def __init__(self, place, full, send, recv, chunks=2):
        self.place, self.full, self.send, self.recv, self.chunks = place, full, send, recv, chunks

    def rows(self, owner, chunk):
        size = self.full.shape[0] // 4
        part = size // self.chunks
        return self.full.at[pl.ds(pl.multiple_of(owner * size + chunk * part, part), part)]

    def copy(self, kind, chunk, owner):
        where = {"mp": self.place.twin if kind == 1 else self.place.mate}
        ref = self.rows(owner, chunk)
        return remote(ref, ref, self.send.at[kind, chunk], self.recv.at[kind, chunk], where)

    def begin(self, chunk):
        self.copy(1, chunk, self.place.m).start()
        self.copy(0, chunk, self.place.m).start()

    def relay(self, chunk):
        self.copy(1, chunk, self.place.twin).wait_recv()
        self.copy(2, chunk, self.place.twin).start()

    def end(self, chunk):
        self.copy(0, chunk, self.place.mate).wait_recv()
        self.copy(2, chunk, self.place.far).wait_recv()

    def finish(self):
        for chunk in range(self.chunks):
            for kind in range(3):
                self.copy(kind, chunk, self.place.m).wait_send()


def norm_scale(values):
    return lax.rsqrt(jnp.mean(values * values, axis=-1, keepdims=True) + EPSILON)


class PairScatter:
    def __init__(self, place, give, got, over, came, send, recv, chunks=2):
        self.place, self.chunks = place, chunks
        self.give, self.got, self.over, self.came = give, got, over, came
        self.send, self.recv = send, recv

    def rows(self, chunk):
        part = self.over.shape[0] // self.chunks
        return pl.ds(chunk * part, part)

    def copy(self, kind, chunk):
        rows = self.rows(chunk)
        if kind == 2:
            source, target, where = self.over.at[rows], self.came.at[rows], {"mp": self.place.twin}
        else:
            source, target, where = self.give.at[kind, rows], self.got.at[kind, rows], {"mp": self.place.mate}
        return remote(source, target, self.send.at[kind, chunk], self.recv.at[kind, chunk], where)

    def far(self, value):
        self.give[0] = value.astype(BF16)
        for chunk in range(self.chunks):
            self.copy(0, chunk).start()

    def twin(self, value):
        part = self.over.shape[0] // self.chunks
        for chunk in range(self.chunks):
            rows = self.rows(chunk)
            self.copy(0, chunk).wait_recv()
            mine = value[chunk * part : (chunk + 1) * part]
            self.over[rows, :] = (mine + self.got[0, rows, :].astype(F32)).astype(BF16)
            self.copy(2, chunk).start()

    def mate(self, value):
        self.give[1] = value.astype(BF16)
        for chunk in range(self.chunks):
            self.copy(1, chunk).start()

    def take(self, chunk, value):
        rows = self.rows(chunk)
        self.copy(1, chunk).wait_recv()
        self.copy(2, chunk).wait_recv()
        return value + self.got[1, rows, :].astype(F32) + self.came[rows, :].astype(F32)

    def finish(self):
        for kind in range(3):
            for chunk in range(self.chunks):
                self.copy(kind, chunk).wait_send()

    @staticmethod
    def scratch(rows, columns, chunks=2):
        return [
            pltpu.VMEM((2, rows, columns), BF16), pltpu.VMEM((2, rows, columns), BF16),
            pltpu.VMEM((rows, columns), BF16), pltpu.VMEM((rows, columns), BF16),
            DMA((3, chunks)), DMA((3, chunks)),
        ]


class RingScatter:
    def __init__(self, place, term, put, inbox, send, recv, last=None):
        self.place, self.term, self.put, self.inbox, self.last = place, term, put, inbox, last
        self.send, self.recv = send, recv
        self.steps = place.n // 2

    def copy(self, way, step):
        source, target = self.put.at[way, step], self.inbox.at[way, step]
        if step == 0:
            half = source.shape[0] // 2
            rows = pl.ds(pl.multiple_of(half * way, half), half)
            source, target = source.at[rows], target.at[rows]
        where = {"dp": self.place.right + way * (self.place.left - self.place.right)}
        return remote(source, target, self.send.at[way, step], self.recv.at[way, step], where)

    def arrived(self, way, step, total):
        self.copy(way, step).wait_recv()
        came = self.inbox[way, step].astype(F32)
        if step == 0:
            row = lax.broadcasted_iota(jnp.int32, came.shape, 0)
            half = came.shape[0] // 2
            came = jnp.where((row >= half * way) & (row < half * way + half), came, 0.0)
        return total + came

    def advance(self, step):
        place, away = self.place, self.steps - step

        @pl.loop(0, 2)
        def _(way):
            owner = place.device(place.pos + place.n + away * (1 - 2 * way))
            total = self.term(owner)
            if step:
                total = self.arrived(way, step - 1, total)
            if step == self.steps - 1 and self.last is not None:
                self.copy(way, 0).wait_send()
                self.put[way, 0] = total.astype(BF16)
            else:
                self.put[way, step] = total.astype(BF16)
                self.copy(way, step).start()

    def total(self):
        total = self.term(self.place.d)
        if self.last is None:
            for way in (0, 1):
                total = self.arrived(way, self.steps - 1, total)
        return total

    def finish(self):
        handed = self.last is not None
        for way in (0, 1):
            for step in range(handed, self.steps - handed):
                self.copy(way, step).wait_send()

    @staticmethod
    def scratch(n, rows, columns, handed=False):
        steps = n // 2 - handed
        return [
            pltpu.VMEM((2, steps, rows, columns), BF16), pltpu.VMEM((2, steps, rows, columns), BF16),
            DMA((2, steps)), DMA((2, steps)),
        ]


def slot_columns(ref, slot, n):
    width = ref.shape[1] // n
    pair = ref[:, pl.ds(pl.multiple_of((slot // 2) * (2 * width), 2 * width), 2 * width)]
    return jnp.where(lax.rem(slot, 2) == 0, pair[:, :width], pair[:, width:])


def gate_terms(gate):
    square = gate * gate
    inner = 0.7978845608 * (gate + 0.044715 * (square * gate))
    bend = jnp.tanh(inner)
    half = 0.5 * (1.0 + bend)
    slope = half + 0.5 * gate * (1.0 - bend * bend) * (0.7978845608 * (1.0 + 0.134145 * square))
    return gate * half, slope


def bucket_onehot(kind, block, count):
    column = lax.broadcasted_iota(jnp.int32, (count, 2 * block), 1)
    offset = jnp.where(column < block, column, column - 2 * block) + (kind - 2) * block
    if kind in (0, KINDS - 1):
        offset = jnp.full_like(column, (kind - 2) * block)
    distance = jnp.abs(offset)
    far_bucket = 7 + sum(((distance >= limit).astype(jnp.int32) for limit in THRESHOLDS))
    bucket = jnp.where(distance < 8, distance, far_bucket) + jnp.where(offset > 0, 16, 0)
    return (bucket == lax.broadcasted_iota(jnp.int32, bucket.shape, 0)).astype(F32)


def bias_tiles(table_ref, tiles_ref):
    heads, kinds, block, _ = tiles_ref.shape
    for t in range(kinds):
        onehot = bucket_onehot(t, block, table_ref.shape[1])
        lines = lax.dot_general(
            table_ref[...], onehot, (((1,), (0,)), ((), ())), precision=HIGHEST, preferred_element_type=F32
        )
        for h in range(heads):
            line = jnp.broadcast_to(lines[h : h + 1, :], (block, 2 * block))
            if t in (0, kinds - 1):
                tiles_ref[h, t] = line[:, :block]
            else:
                tiles_ref[h, t] = pltpu.roll(line, 0, 1, stride=1, stride_axis=0)[:, :block]


def key_window(seg_smem, index, block, count):
    first, last = seg_smem[0, index * block], seg_smem[0, index * block + block - 1]
    low, high = jnp.int32(0), jnp.int32(0)
    for j in range(count):
        low += (seg_smem[0, j * block + block - 1] < first).astype(jnp.int32)
        high += (seg_smem[0, j * block] <= last).astype(jnp.int32)
    return low, high - low


def segment_column(segr_ref):
    return jnp.broadcast_to(segr_ref[...].astype(F32), (8, segr_ref.shape[1])).T


def window_blocks(segr_ref, segc_ref, rows, index, low, blocks, block):
    places, sames, tile_at = [], [], []
    for t in range(blocks):
        j = low + t
        place = pl.ds(pl.multiple_of(j * block, block), block)
        places.append(place)
        sames.append(segc_ref[rows, 0:1] == segr_ref[:, place].astype(F32))
        tile_at.append(jnp.clip(j - index, -2, 2) + 2)
    return places, sames, tile_at


def score_block(query, key_rows, tile, same):
    return jnp.where(same, matmul_nt(query, key_rows) + tile, MASKED)


def attend_kernel(seg_smem, qkv_ref, segr_ref, tiles_ref, ctx_ref, ctx32_ref, lse_ref, segc_ref):
    heads, _, block, _ = tiles_ref.shape
    length, width = qkv_ref.shape
    width = width // (3 * heads)
    count = length // block
    segc_ref[...] = segment_column(segr_ref)

    def run(index, low, blocks):
        rows = pl.ds(pl.multiple_of(index * block, block), block)
        places, sames, tile_at = window_blocks(segr_ref, segc_ref, rows, index, low, blocks, block)
        outs, logs = [], []
        for h in range(heads):
            lanes = slice(h * width, (h + 1) * width)
            query = qkv_ref[rows, :][:, lanes]
            scores = []
            for t in range(blocks):
                key_rows = qkv_ref[places[t], :][:, heads * width + h * width : heads * width + (h + 1) * width]
                scores.append(score_block(query, key_rows, tiles_ref[h, tile_at[t]], sames[t]))
            peak = functools.reduce(jnp.maximum, scores)
            peak = jnp.max(peak, axis=1, keepdims=True)
            raised = [jnp.exp(s - peak) for s in scores]
            total = jnp.sum(functools.reduce(jnp.add, raised), axis=1, keepdims=True)
            scale = 1.0 / total
            context = jnp.zeros((block, width), F32)
            for t in range(blocks):
                value_rows = qkv_ref[places[t], :][:, 2 * heads * width + h * width : 2 * heads * width + (h + 1) * width]
                context += matmul((raised[t] * scale).astype(BF16), value_rows)
            outs.append(context)
            logs.append(peak + jnp.log(total))
        context = jnp.concatenate(outs, axis=1)
        ctx32_ref[rows, :] = context
        ctx_ref[rows, :] = context.astype(BF16)
        lse_ref[rows, :] = jnp.concatenate(logs + [jnp.zeros((block, 8 - heads), F32)], axis=1)

    @pl.loop(0, count)
    def _(index):
        low, many = key_window(seg_smem, index, block, count)
        for blocks in range(1, count + 1):
            pl.when(many == blocks)(functools.partial(run, index, low, blocks))


def attend(qkv, segments, tiles):
    length, width = qkv.shape
    heads = tiles.shape[0]
    return pl.pallas_call(
        attend_kernel,
        name="attend",
        out_shape=(
            jax.ShapeDtypeStruct((length, width // 3), BF16),
            jax.ShapeDtypeStruct((length, width // 3), F32),
            jax.ShapeDtypeStruct((length, 8), F32),
        ),
        in_specs=[pl.BlockSpec(memory_space=pltpu.SMEM)] + [VMEM_SPEC] * 3,
        out_specs=(VMEM_SPEC,) * 3,
        scratch_shapes=[pltpu.VMEM((length, 8), F32)],
        cost_estimate=pl.CostEstimate(flops=2 * length * length * width, bytes_accessed=8 << 20, transcendentals=heads * length * length),
    )(segments, qkv, segments, tiles)


def attend_back_kernel(
    seg_smem, qkv_ref, segr_ref, tiles_ref, ctx32_ref, lse_ref, mixed_ref, wmix_ref,
    cots_ref, table_ref, segc_ref, do_ref, dk_ref, dv_ref, sums_ref,
):
    heads, kinds, block, _ = tiles_ref.shape
    length, width = qkv_ref.shape
    width = width // (3 * heads)
    count = length // block
    segc_ref[...] = segment_column(segr_ref)
    dk_ref[...] = jnp.zeros_like(dk_ref)
    dv_ref[...] = jnp.zeros_like(dv_ref)
    sums_ref[...] = jnp.zeros_like(sums_ref)

    @pl.loop(0, count)
    def _(index):
        rows = pl.ds(pl.multiple_of(index * block, block), block)
        weight = wmix_ref[...].reshape(-1, heads * width)
        do_ref[rows, :] = matmul(mixed_ref[rows, :], weight).astype(BF16)

    def run(index, low, blocks):
        rows = pl.ds(pl.multiple_of(index * block, block), block)
        places, sames, tile_at = window_blocks(segr_ref, segc_ref, rows, index, low, blocks, block)
        product = do_ref[rows, :].astype(F32) * ctx32_ref[rows, :]
        logs = lse_ref[rows, :]
        outs = []
        for h in range(heads):
            lanes = slice(h * width, (h + 1) * width)
            query = qkv_ref[rows, :][:, lanes]
            grad = do_ref[rows, :][:, lanes]
            inner = jnp.sum(product[:, lanes], axis=1, keepdims=True)
            log = logs[:, h : h + 1]
            query_cot = jnp.zeros((block, width), F32)
            for t in range(blocks):
                here = qkv_ref[places[t], :]
                key_rows = here[:, heads * width + h * width : heads * width + (h + 1) * width]
                value_rows = here[:, 2 * heads * width + h * width : 2 * heads * width + (h + 1) * width]
                probs = jnp.exp(score_block(query, key_rows, tiles_ref[h, tile_at[t]], sames[t]) - log)
                prob_cot = matmul_nt(grad, value_rows)
                cot = (probs * (prob_cot - inner)).astype(BF16)
                dv_ref[h, places[t], :] += matmul_tn(probs.astype(BF16), grad)
                dk_ref[h, places[t], :] += matmul_tn(cot, query)
                query_cot += matmul(cot, key_rows)
                sums_ref[h, tile_at[t]] += cot.astype(F32)
            outs.append(query_cot)
        cots_ref[rows, : heads * width] = jnp.concatenate(outs, axis=1).astype(BF16)

    @pl.loop(0, count)
    def _(index):
        low, many = key_window(seg_smem, index, block, count)
        for blocks in range(1, count + 1):
            pl.when(many == blocks)(functools.partial(run, index, low, blocks))

    both = [dk_ref[h] for h in range(heads)] + [dv_ref[h] for h in range(heads)]
    cots_ref[:, heads * width :] = jnp.concatenate(both, axis=1).astype(BF16)
    near = [(h, t) for h in range(heads) for t in range(1, kinds - 1)]

    def shifted(group, totals):
        rows = pl.ds(pl.multiple_of(group * 8, 8), 8)
        amount = lax.rem(2 * block - 8 * group, 2 * block)
        out = []
        for (h, t), total in zip(near, totals):
            eight = sums_ref[h, t, rows, :]
            wide = jnp.concatenate([eight, jnp.zeros_like(eight)], axis=1)
            out.append(total + pltpu.roll(wide, amount, 1))
        return tuple(out)

    empty = jnp.zeros((8, 2 * block), F32)
    totals = dict(zip(near, lax.fori_loop(0, block // 8, shifted, (empty,) * len(near))))
    place = lax.broadcasted_iota(jnp.int32, empty.shape, 0)
    result = jnp.zeros(table_ref.shape, F32)
    for t in range(kinds):
        lines = []
        for h in range(heads):
            if (h, t) in totals:
                total = totals[h, t]
                for bit in (1, 2, 4):
                    total = jnp.where((place // bit) % 2 == 1, pltpu.roll(total, 2 * block - bit, 1), total)
                lines.append(jnp.sum(total, axis=0, keepdims=True))
            else:
                line = jnp.sum(sums_ref[h, t], axis=0, keepdims=True)
                lines.append(jnp.concatenate([line, jnp.zeros_like(line)], axis=1))
        lines.append(jnp.zeros((8 - heads, 2 * block), F32))
        result += lax.dot_general(
            jnp.concatenate(lines, axis=0), bucket_onehot(t, block, 128),
            (((1,), (1,)), ((), ())), precision=HIGHEST, preferred_element_type=F32,
        )
    table_ref[...] = result


def attend_back(qkv, segments, tiles, ctx32, lse, mixed, wmix):
    length, width = qkv.shape
    heads, _, block, _ = tiles.shape
    size = width // (3 * heads)
    return pl.pallas_call(
        attend_back_kernel,
        name="attend_back",
        out_shape=(
            jax.ShapeDtypeStruct((length, width), BF16),
            jax.ShapeDtypeStruct((8, 128), F32),
        ),
        in_specs=[pl.BlockSpec(memory_space=pltpu.SMEM)] + [VMEM_SPEC] * 7,
        out_specs=(VMEM_SPEC,) * 2,
        cost_estimate=pl.CostEstimate(flops=8 * length * length * width, bytes_accessed=32 << 20, transcendentals=heads * length * length),
        scratch_shapes=[
            pltpu.VMEM((length, 8), F32),
            pltpu.VMEM((length, width // 3), BF16),
            pltpu.VMEM((heads, length, size), F32),
            pltpu.VMEM((heads, length, size), F32),
            pltpu.VMEM((heads, 5, block, block), F32),
        ],
    )(segments, qkv, segments, tiles, ctx32, lse, mixed, wmix)


def block_rows(owner, size):
    return pl.ds(pl.multiple_of(owner * size, size), size)


def gain_lanes(n, shape):
    row = lax.broadcasted_iota(jnp.int32, shape, 0)
    lane = lax.broadcasted_iota(jnp.int32, shape, 1)
    count = shape[1] // (4 * n)
    shift = (row // 8) * count
    inside = (lane >= shift) & (lane < shift + count)
    return inside, row - 8 * (row // 8)


def gain_spread(n, features):
    count = features // (4 * n)
    lane = lax.broadcasted_iota(jnp.int32, (128, features), 1)
    row = lax.broadcasted_iota(jnp.int32, (128, features), 0)
    share = ((lane.astype(F32) + 0.5) * (1.0 / count)).astype(jnp.int32)
    return (lane - share * count == row).astype(F32)


def widened(part, width):
    spare = width - part.shape[1]
    part = part.astype(BF16)
    if spare:
        part = jnp.concatenate([part, jnp.zeros((part.shape[0], spare), BF16)], axis=1)
    return part


def flat(ref):
    return ref[...].reshape(-1, ref.shape[2])


def transpose_slots(source, target):
    n, width, _ = target.shape
    for pair in range(n // 2):
        both = source[:, 2 * width * pair : 2 * width * (pair + 1)].T
        target[2 * pair] = both[:width]
        target[2 * pair + 1] = both[width:]


def enter_kernel(
    n, x_ref, cot_ref, gain_ref, gain_two_ref, wq_ref, wk_ref, wv_ref, wm_ref, wg_ref, wl_ref, wd_ref, table_ref,
    normed_out, cot_out, wgate_out, qkv_out, wqkv_out, wmix_out, tiles_out, lift_ref, down_ref, gains_ref,
    wfull, gfull, nfull, cfull, normed_t, cot_t, g1, g4, g32, qkv_v, wqkv_v, wmix_v, tiles_v,
    ring_send, ring_recv, gate_send, gate_recv, pair_send, pair_recv, cot_send, cot_recv,
    g_send, g_recv, h_send, h_recv, local_sem, out_sem,
):
    place = Place(n)
    size, features = x_ref.shape
    per = gain_ref.shape[0]
    wide = gfull.shape[2]
    heads = wq_ref.shape[1]
    g1[...] = jnp.zeros_like(g1)
    g1[0:1, 0:per] = gain_ref[...].reshape(1, per)
    g1[1:2, 0:per] = gain_two_ref[...].reshape(1, per)
    for k, ref in enumerate((wq_ref, wk_ref, wv_ref)):
        wfull[place.d, :, k * heads : (k + 1) * heads] = ref[...].astype(BF16)
    wfull[place.d, :, 3 * heads :] = wm_ref[...].T.astype(BF16)
    gfull[place.d] = widened(wg_ref[...], wide)
    own_g = pltpu.make_async_copy(g1, g4.at[place.m], local_sem.at[0])
    own_g.start()
    place.barrier(everyone=True)
    ring = RingGather(place, wfull, ring_send, ring_recv)
    gate_ring = RingGather(place, gfull, gate_send, gate_recv)
    small = [
        remote(g1, g4.at[place.m], g_send.at[k], g_recv.at[k], {"mp": lax.rem(place.m + k, 4)})
        for k in range(1, 4)
    ]
    for copy in small:
        copy.start()

    def both(which, step):
        for way in (0, 1):
            which.advance(way, step)

    both(ring, 0)
    both(gate_ring, 0)
    scale = norm_scale(x_ref[...])
    rows = block_rows(place.m, size)
    own_g.wait()
    for k in range(1, 4):
        slot = g4.at[lax.rem(place.m + 4 - k, 4)]
        remote(slot, slot, g_send.at[k], g_recv.at[k], {"mp": place.mate}).wait_recv()
    around = [
        remote(g4, g32.at[place.d], h_send.at[k], h_recv.at[k], {"dp": lax.rem(place.d + k, n)})
        for k in range(1, n)
    ]
    for copy in around:
        copy.start()
    own_h = pltpu.make_async_copy(g4, g32.at[place.d], local_sem.at[0])
    own_h.start()
    cfull[rows, :] = cot_ref[...].astype(BF16)
    spread = gain_spread(n, features).astype(BF16)
    own_h.wait()
    for k in range(1, n):
        slot = g32.at[lax.rem(place.d + n - k, n)]
        remote(g4, slot, h_send.at[k], h_recv.at[k], {"dp": place.right}).wait_recv()
    pieces = g32[...].reshape(-1, 128).astype(BF16)
    spaced = matmul(pieces, spread)
    inside, kind = gain_lanes(n, spaced.shape)
    gain = jnp.sum(jnp.where(inside & (kind == 0), spaced, 0.0), axis=0, keepdims=True)
    gain_two = jnp.sum(jnp.where(inside & (kind == 1), spaced, 0.0), axis=0, keepdims=True)
    nfull[rows, :] = (x_ref[...] * scale * gain).astype(BF16)
    pair = PairGather(place, nfull, pair_send, pair_recv)
    cots = PairGather(place, cfull, cot_send, cot_recv)
    for chunk in range(2):
        pair.begin(chunk)
    for chunk in range(2):
        cots.begin(chunk)
    gains_ref[...] = jnp.concatenate([gain, gain_two] + [jnp.zeros_like(gain)] * 6, axis=0)
    both(ring, 1)
    lift_ref[...] = widened(wl_ref[...], wide)
    down_ref[...] = widened(wd_ref[...], wide)
    both(gate_ring, 1)
    pair.relay(0)
    bias_tiles(table_ref, tiles_v)
    out_t = pltpu.make_async_copy(tiles_v, tiles_out, out_sem.at[0])
    out_t.start()
    both(ring, 2)
    pair.relay(1)
    both(gate_ring, 2)
    for chunk in range(2):
        pair.end(chunk)
    transpose_slots(nfull, normed_t)
    out_n = pltpu.make_async_copy(normed_t, normed_out, out_sem.at[1])
    out_n.start()
    both(ring, 3)
    both(gate_ring, 3)
    cots.relay(0)
    for step in range(4, n // 2 + 1):
        both(ring, step)
    wqkv_v[...] = wfull[:, :, : 3 * heads]
    wmix_v[...] = wfull[:, :, 3 * heads :]
    out_w = pltpu.make_async_copy(wqkv_v, wqkv_out, out_sem.at[2])
    out_m = pltpu.make_async_copy(wmix_v, wmix_out, out_sem.at[3])
    out_w.start()
    out_m.start()

    @pl.loop(0, 4)
    def _(block):
        rows = block_rows(block, size)
        qkv_v[rows, :] = matmul(nfull[rows, :], flat(wqkv_v)).astype(BF16)

    out_q = pltpu.make_async_copy(qkv_v, qkv_out, out_sem.at[4])
    out_q.start()
    cots.relay(1)
    for chunk in range(2):
        cots.end(chunk)
    transpose_slots(cfull, cot_t)
    out_c = pltpu.make_async_copy(cot_t, cot_out, out_sem.at[6])
    out_c.start()
    for step in range(4, n // 2 + 1):
        both(gate_ring, step)
    out_g = pltpu.make_async_copy(gfull, wgate_out, out_sem.at[5])
    out_g.start()
    ring.finish()
    gate_ring.finish()
    pair.finish()
    cots.finish()
    for copy in small + around:
        copy.wait_send()
    for copy in (out_t, out_n, out_w, out_m, out_q, out_g, out_c):
        copy.wait()


def enter(n, x, cot, gain, gain_two, wq, wk, wv, wm, wg, wl, wd, table):
    size, features = x.shape
    rows, heads = wq.shape
    wide = wg.shape[1] + -wg.shape[1] % 128
    count = table.shape[0]
    shape = jax.ShapeDtypeStruct
    outs = (
        shape((n, features // n, 4 * size), BF16),
        shape((n, features // n, 4 * size), BF16),
        shape((n, rows, wide), BF16),
        shape((4 * size, 3 * heads), BF16),
        shape((n, rows, 3 * heads), BF16),
        shape((n, rows, heads), BF16),
        shape((count, KINDS, BLOCK, BLOCK), F32),
        shape((rows, wide), BF16),
        shape((rows, wide), BF16),
        shape((8, features), F32),
    )
    return pl.pallas_call(
        functools.partial(enter_kernel, n),
        name="enter",
        out_shape=outs,
        in_specs=[VMEM_SPEC] * 12,
        out_specs=(ANY_SPEC,) * 7 + (VMEM_SPEC,) * 3,
        scratch_shapes=[
            pltpu.VMEM((n, rows, 4 * heads), BF16),
            pltpu.VMEM((n, rows, wide), BF16),
            pltpu.VMEM((4 * size, features), BF16),
            pltpu.VMEM((4 * size, features), BF16),
            pltpu.VMEM(outs[0].shape, BF16),
            pltpu.VMEM(outs[1].shape, BF16),
            pltpu.VMEM((8, 128), F32),
            pltpu.VMEM((4, 8, 128), F32),
            pltpu.VMEM((n, 4, 8, 128), F32),
            *(pltpu.VMEM(outs[k].shape, outs[k].dtype) for k in (3, 4, 5, 6)),
            DMA((2, n // 2)), DMA((2, n // 2)),
            DMA((2, n // 2)), DMA((2, n // 2)),
            DMA((3, 2)), DMA((3, 2)),
            DMA((3, 2)), DMA((3, 2)),
            DMA((4,)), DMA((4,)),
            DMA((n,)), DMA((n,)),
            DMA((1,)), DMA((7,)),
        ],
        compiler_params=pltpu.CompilerParams(collective_id=0, has_side_effects=True),
    )(x, cot, gain, gain_two, wq, wk, wv, wm, wg, wl, wd, table)


def middle_kernel(
    n, ctx_ref, wmix_ref, x_ref, gains_ref, lift_ref, from_left_ref, from_right_ref, down_ref, wgate_any,
    second_out, lift_out, down_out, bend_out, slope_out, hidden_out, middle_ref,
    lfull, dfull, gate_v, sfull, second_t, own_v, bend_v, slope_v, hidden_v,
    give, got, over, came, sc_send, sc_recv,
    pair_send, pair_recv, lift_send, lift_recv, down_send, down_recv, local_sem, out_sem,
):
    place = Place(n)
    size = x_ref.shape[0]
    starts = [
        pltpu.make_async_copy(source, target, local_sem.at[k])
        for k, (source, target) in enumerate(
            (
                (from_left_ref, lfull.at[place.left]),
                (from_right_ref, lfull.at[place.right]),
                (lift_ref, lfull.at[place.d]),
                (down_ref, dfull.at[place.d]),
                (wgate_any, gate_v),
            )
        )
    ]
    for copy in starts:
        copy.start()
    place.barrier()
    lift = RingGather(place, lfull, lift_send, lift_recv, first=1)
    down = RingGather(place, dfull, down_send, down_recv)
    scatter = PairScatter(place, give, got, over, came, sc_send, sc_recv)
    pair = PairGather(place, sfull, pair_send, pair_recv)

    def both(ring, step):
        for way in (0, 1):
            ring.advance(way, step)

    for copy in starts[:4]:
        copy.wait()
    both(lift, 1)
    both(down, 0)

    def part(owner):
        return matmul_nt(ctx_ref[block_rows(owner, size), :], flat(wmix_ref))

    scatter.far(part(place.far))
    scatter.twin(part(place.twin))
    scatter.mate(part(place.mate))
    own_v[...] = part(place.m)
    both(lift, 2)
    gain = gains_ref[1:2, :]
    chunk_rows = size // 2
    for chunk in range(2):
        rows = slice(chunk * chunk_rows, (chunk + 1) * chunk_rows)
        middle = x_ref[rows, :] + scatter.take(chunk, own_v[rows, :])
        middle_ref[rows, :] = middle
        start = pl.multiple_of(place.m * size + chunk * chunk_rows, chunk_rows)
        sfull[pl.ds(start, chunk_rows), :] = (middle * norm_scale(middle) * gain).astype(BF16)
        pair.begin(chunk)
    both(down, 1)
    starts[4].wait()

    def gate_block(k, _=None):
        rows = block_rows(lax.rem(place.m + k, 4), size)
        bend, slope = gate_terms(matmul(sfull[rows, :], flat(gate_v)))
        bend_v[rows, :] = bend
        slope_v[rows, :] = slope

    @pl.loop(0, 4)
    def _(k):
        @pl.when(k == 1)
        def _():
            both(lift, 3)
            pair.relay(0)
            both(down, 2)
            pair.relay(1)
            for chunk in range(2):
                pair.end(chunk)

        gate_block(k)

    transpose_slots(sfull, second_t)
    out_s = pltpu.make_async_copy(second_t, second_out, out_sem.at[0])
    out_b = pltpu.make_async_copy(bend_v, bend_out, out_sem.at[1])
    out_s.start()
    out_b.start()
    for step in range(4, n // 2 + 1):
        both(lift, step)
    out_l = pltpu.make_async_copy(lfull, lift_out, out_sem.at[2])
    out_l.start()
    both(down, 3)

    @pl.loop(0, 4)
    def _(k):
        rows = block_rows(k, size)
        lifted = matmul(sfull[rows, :], flat(lfull))
        hidden_v[rows, :] = (bend_v[rows, :] * lifted).astype(BF16)
        slope_v[rows, :] = slope_v[rows, :] * lifted

    out_p = pltpu.make_async_copy(slope_v, slope_out, out_sem.at[3])
    out_h = pltpu.make_async_copy(hidden_v, hidden_out, out_sem.at[4])
    out_d = pltpu.make_async_copy(dfull, down_out, out_sem.at[5])
    out_p.start()
    out_h.start()
    for step in range(4, n // 2 + 1):
        both(down, step)
    out_d.start()
    lift.finish()
    down.finish()
    scatter.finish()
    pair.finish()
    for copy in (out_s, out_b, out_l, out_p, out_h, out_d):
        copy.wait()


def middle_part(n, ctx, wmix, x, gains, lift, from_left, from_right, down, wgate):
    size, features = x.shape
    rows, wide = lift.shape
    length = 4 * size
    shape = jax.ShapeDtypeStruct
    full = shape((n, rows, wide), BF16)
    return pl.pallas_call(
        functools.partial(middle_kernel, n),
        name="middle",
        out_shape=(
            shape((n, features // n, length), BF16),
            full,
            full,
            shape((length, wide), F32),
            shape((length, wide), F32),
            shape((length, wide), BF16),
            shape((size, features), F32),
        ),
        in_specs=[VMEM_SPEC] * 8 + [ANY_SPEC],
        out_specs=(ANY_SPEC,) * 6 + (VMEM_SPEC,),
        scratch_shapes=[
            pltpu.VMEM((n, rows, wide), BF16),
            pltpu.VMEM((n, rows, wide), BF16),
            pltpu.VMEM((n, rows, wide), BF16),
            pltpu.VMEM((length, features), BF16),
            pltpu.VMEM((n, features // n, length), BF16),
            pltpu.VMEM((size, features), F32),
            pltpu.VMEM((length, wide), F32),
            pltpu.VMEM((length, wide), F32),
            pltpu.VMEM((length, wide), BF16),
            *PairScatter.scratch(size, features),
            DMA((3, 2)), DMA((3, 2)),
            DMA((2, n // 2)), DMA((2, n // 2)),
            DMA((2, n // 2)), DMA((2, n // 2)),
            DMA((5,)), DMA((6,)),
        ],
        compiler_params=pltpu.CompilerParams(collective_id=1, has_side_effects=True),
    )(ctx, wmix, x, gains, lift, from_left, from_right, down, wgate)


def norm_back(values, gain, grad):
    scale = norm_scale(values)
    term = grad * values
    inner = jnp.mean(term * gain, axis=-1, keepdims=True)
    return gain * scale * grad - values * (scale * scale * scale * inner), term * scale


def back_kernel(
    n, middle_ref, gains_ref, cotangent_any, hidden_any, cot_any, second_any, bend_any, slope_any, wgate_any, wlift_any, wdown_any,
    mixed_out, pending_out, output_out, middle_cot_out, feed_ref, own_ref,
    hidden_v, cot_v, gate_v, lift_v, down_v, bend_v, slope_v, gcot_v, lcot_v, mixed_v, part_v, part_two_v,
    give, got, over, came, sc_send, sc_recv,
    give_two, got_two, over_two, came_two, sd_send, sd_recv,
    pair_send, pair_recv,
    put_g, in_g, send_g, recv_g, put_l, in_l, send_l, recv_l, put_d, in_d, send_d, recv_d,
    load_sem, piece_sem, pend_sem, out_sem,
):
    place = Place(n)
    size = middle_ref.shape[0]
    loads = [
        pltpu.make_async_copy(source, target, load_sem.at[k])
        for k, (source, target) in enumerate(
            ((hidden_any, hidden_v), (cot_any, cot_v), (wdown_any, down_v), (wgate_any, gate_v), (wlift_any, lift_v), (cotangent_any, part_two_v))
        )
    ]
    for copy in loads:
        copy.start()

    def owner_of(k):
        core = lax.rem(place.m + 3 - k, 2)
        chip = lax.rem(place.m // 2 + (3 - k) // 2, 2)
        return 2 * chip + core

    def pieces(k):
        rows = block_rows(owner_of(k), size)
        return [
            pltpu.make_async_copy(source.at[rows], target.at[lax.rem(k, 2)], piece_sem.at[lax.rem(k, 2), i])
            for i, (source, target) in enumerate(((bend_any, bend_v), (slope_any, slope_v)))
        ]

    for copy in pieces(0):
        copy.start()
    place.barrier()
    gate = RingScatter(place, lambda slot: matmul(gate_v[slot], gcot_v[...]), put_g, in_g, send_g, recv_g, 0)
    lift = RingScatter(place, lambda slot: matmul(gate_v[slot], lcot_v[...]), put_l, in_l, send_l, recv_l, 1)
    down = RingScatter(place, lambda slot: matmul(cot_v[slot], hidden_v[...]), put_d, in_d, send_d, recv_d, 2)
    scatter = PairScatter(place, give, got, over, came, sc_send, sc_recv)
    downs = PairScatter(place, give_two, got_two, over_two, came_two, sd_send, sd_recv)
    pair = PairGather(place, mixed_v, pair_send, pair_recv)

    def hand(ring):
        return [
            pltpu.make_async_copy(ring.put.at[way, 0], pending_out.at[way, ring.last], pend_sem.at[ring.last, way])
            for way in (0, 1)
        ]

    loads[0].wait()
    loads[1].wait()
    down.advance(0)
    for copy in loads[2:5]:
        copy.wait()

    @pl.loop(0, 4)
    def _(k):
        rows = block_rows(owner_of(k), size)

        @pl.when(k < 3)
        def _():
            for copy in pieces(k + 1):
                copy.start()

        hidden_cot = matmul_tn(cot_v[:, :, rows].reshape(-1, size), flat(down_v))
        for copy in pieces(k):
            copy.wait()
        gcot_v[rows, :] = (hidden_cot * slope_v[lax.rem(k, 2)]).astype(BF16)
        lcot_v[rows, :] = (hidden_cot * bend_v[lax.rem(k, 2)]).astype(BF16)
        part_v[...] = matmul_nt(gcot_v[rows, :], flat(gate_v)) + matmul_nt(lcot_v[rows, :], flat(lift_v))

        @pl.when(k == 0)
        def _():
            scatter.far(part_v[...])

        @pl.when(k == 1)
        def _():
            scatter.twin(part_v[...])
            down.advance(1)

        @pl.when(k == 2)
        def _():
            scatter.mate(part_v[...])

    load_second = pltpu.make_async_copy(second_any, gate_v, load_sem.at[3])
    load_second.start()
    down.advance(2)
    load_second.wait()
    gate.advance(0)
    lift.advance(0)
    loads[5].wait()
    chunk_rows = size // 2
    gain = gains_ref[1:2, :]
    feed = jnp.zeros_like(gain)
    for chunk in range(2):
        rows = slice(chunk * chunk_rows, (chunk + 1) * chunk_rows)
        grad = scatter.take(chunk, part_v[rows, :])
        through, term = norm_back(middle_ref[rows, :], gain, grad)
        middle_cot = part_two_v[rows, :] + through
        part_v[rows, :] = middle_cot
        feed += jnp.sum(term, axis=0, keepdims=True)
        start = pl.multiple_of(place.m * size + chunk * chunk_rows, chunk_rows)
        mixed_v[pl.ds(start, chunk_rows), :] = middle_cot.astype(BF16)
        pair.begin(chunk)
    out_c = pltpu.make_async_copy(part_v, middle_cot_out, out_sem.at[0])
    out_c.start()
    feed_ref[...] = jnp.concatenate([feed] + [jnp.zeros_like(feed)] * 7, axis=0)
    gate.advance(1)
    down.advance(3)
    for copy in hand(down):
        copy.start()
    lift.advance(1)

    @pl.loop(0, 4)
    def _(k):
        part_two_v[...] = matmul_nt(hidden_v[block_rows(owner_of(k), size), :], flat(down_v))

        @pl.when(k == 0)
        def _():
            downs.far(part_two_v[...])

        @pl.when(k == 1)
        def _():
            downs.twin(part_two_v[...])

        @pl.when(k == 2)
        def _():
            downs.mate(part_two_v[...])

    pair.relay(0)
    pair.relay(1)
    gate.advance(2)
    own_ref[2] = down.total()
    lift.advance(2)
    for chunk in range(2):
        pair.end(chunk)
    out_m = pltpu.make_async_copy(mixed_v, mixed_out, out_sem.at[1])
    out_m.start()
    own_ref[0] = gate.total()
    own_ref[1] = lift.total()
    for chunk in range(2):
        rows = slice(chunk * chunk_rows, (chunk + 1) * chunk_rows)
        part_two_v[rows, :] = middle_ref[rows, :] + downs.take(chunk, part_two_v[rows, :])
    out_o = pltpu.make_async_copy(part_two_v, output_out, out_sem.at[2])
    out_o.start()
    gate.advance(3)
    for copy in hand(gate):
        copy.start()
    lift.advance(3)
    for copy in hand(lift):
        copy.start()
    for ring in (gate, lift, down):
        ring.finish()
        for copy in hand(ring):
            copy.wait()
    scatter.finish()
    downs.finish()
    pair.finish()
    out_c.wait()
    out_m.wait()
    out_o.wait()


def back_part(n, middle, cotangent, gains, hidden, cot, second, bend, slope, wgate, wlift, wdown):
    size, features = middle.shape
    length, wide = hidden.shape
    rows = wgate.shape[1]
    shape = jax.ShapeDtypeStruct
    weight = pltpu.VMEM((n, rows, wide), BF16)
    return pl.pallas_call(
        functools.partial(back_kernel, n),
        name="back",
        out_shape=(
            shape((length, features), BF16),
            shape((2, 3, rows, wide), BF16),
            shape((size, features), F32),
            shape((size, features), F32),
            shape((8, features), F32),
            shape((3, rows, wide), F32),
        ),
        in_specs=[VMEM_SPEC] * 2 + [ANY_SPEC] * 9,
        out_specs=(ANY_SPEC,) * 4 + (VMEM_SPEC,) * 2,
        scratch_shapes=[
            pltpu.VMEM((length, wide), BF16),
            pltpu.VMEM((n, features // n, length), BF16),
            weight, weight, weight,
            pltpu.VMEM((2, size, wide), F32),
            pltpu.VMEM((2, size, wide), F32),
            pltpu.VMEM((length, wide), BF16),
            pltpu.VMEM((length, wide), BF16),
            pltpu.VMEM((length, features), BF16),
            pltpu.VMEM((size, features), F32),
            pltpu.VMEM((size, features), F32),
            *PairScatter.scratch(size, features),
            *PairScatter.scratch(size, features),
            DMA((3, 2)), DMA((3, 2)),
            *RingScatter.scratch(n, rows, wide, 1),
            *RingScatter.scratch(n, rows, wide, 1),
            *RingScatter.scratch(n, rows, wide, 1),
            DMA((6,)), DMA((2, 2)), DMA((3, 2)), DMA((3,)),
        ],
        compiler_params=pltpu.CompilerParams(collective_id=2, has_side_effects=True, vmem_limit_bytes=67043328),
    )(middle, gains, cotangent, hidden, cot, second, bend, slope, wgate, wlift, wdown)


def leave_kernel(
    n, cots_ref, ctx_ref, wqkv_ref, x_ref, gains_ref, middle_cot_ref, feed_ref, table_ref, normed_any, mixed_any,
    grad_ref, gain_out, table_out, input_ref,
    normed_v, mixed_v, own_v,
    give, got, over, came, sc_send, sc_recv,
    put, inbox, ring_send, ring_recv,
    tables, pieces_v, spare_v, sum_v, last_v,
    t_send, t_recv, g_send, g_recv, h_send, h_recv, load_sem,
):
    place = Place(n)
    size, features = x_ref.shape
    load_n = pltpu.make_async_copy(normed_any, normed_v, load_sem.at[0])
    load_m = pltpu.make_async_copy(mixed_any, mixed_v, load_sem.at[1])
    load_n.start()
    load_m.start()
    place.barrier(everyone=True)

    def peer(k):
        return {"dp": lax.rem(place.d + k, n)}

    table_copies = [remote(table_ref, tables.at[n - k], t_send.at[k], t_recv.at[k], peer(k)) for k in range(1, n)]
    for copy in table_copies:
        copy.start()
    scatter = PairScatter(place, give, got, over, came, sc_send, sc_recv)

    def term(slot):
        left = matmul(normed_v[slot], cots_ref[...])
        return jnp.concatenate([left, matmul_tn(slot_columns(mixed_v, slot, n), ctx_ref[...])], axis=1)

    ring = RingScatter(place, term, put, inbox, ring_send, ring_recv)

    def part(owner):
        return matmul_nt(cots_ref[block_rows(owner, size), :], flat(wqkv_ref))

    scatter.far(part(place.far))
    load_n.wait()
    load_m.wait()
    ring.advance(0)
    scatter.twin(part(place.twin))
    scatter.mate(part(place.mate))
    ring.advance(1)
    own_v[...] = part(place.m)
    spread = gain_spread(n, features)
    ring.advance(2)
    chunk_rows = size // 2
    gain = gains_ref[0:1, :]
    total = jnp.zeros_like(gain)
    for chunk in range(2):
        rows = slice(chunk * chunk_rows, (chunk + 1) * chunk_rows)
        grad = scatter.take(chunk, own_v[rows, :])
        through, terms = norm_back(x_ref[rows, :], gain, grad)
        input_ref[rows, :] = middle_cot_ref[rows, :] + through
        total += jnp.sum(terms, axis=0, keepdims=True)
    inside, kind = gain_lanes(n, (n * 4 * 8, features))
    rows = jnp.where(inside & (kind == 0), total, 0.0) + jnp.where(inside & (kind == 1), feed_ref[0:1, :], 0.0)
    rows = lax.dot_general(rows, spread, (((1,), (1,)), ((), ())), precision=HIGHEST, preferred_element_type=F32)
    pieces_v[...] = rows.reshape(pieces_v.shape)
    around = [remote(pieces_v.at[lax.rem(place.d + k, n)], spare_v.at[n - k], g_send.at[k], g_recv.at[k], peer(k)) for k in range(1, n)]
    for copy in around:
        copy.start()
    ring.advance(3)
    table = table_ref[...]
    for k in range(1, n):
        remote(table_ref, tables.at[n - k], t_send.at[k], t_recv.at[k], peer(k)).wait_recv()
        table += tables[n - k]
    table_out[...] = table
    sums = pieces_v[place.d]
    for k in range(1, n):
        remote(pieces_v.at[0], spare_v.at[n - k], g_send.at[k], g_recv.at[k], peer(k)).wait_recv()
        sums += spare_v[n - k]
    sum_v[...] = sums
    last = []
    for k in range(1, 4):
        target = lax.rem(place.m + k, 4)
        last.append(remote(sum_v.at[target], last_v.at[4 - k], h_send.at[k], h_recv.at[k], {"mp": target}))
        last[-1].start()
    grad_ref[...] = ring.total()
    sums = sum_v[place.m]
    for k in range(1, 4):
        remote(sum_v.at[0], last_v.at[4 - k], h_send.at[k], h_recv.at[k], {"mp": place.mate}).wait_recv()
        sums += last_v[4 - k]
    gain_out[...] = sums
    ring.finish()
    scatter.finish()
    for copy in table_copies + around + last:
        copy.wait_send()


def leave_part(n, cots, ctx, wqkv, x, gains, middle_cot, feed, table, normed, mixed):
    size, features = x.shape
    length, width = cots.shape
    rows = wqkv.shape[1]
    columns = width + ctx.shape[1]
    shape = jax.ShapeDtypeStruct
    return pl.pallas_call(
        functools.partial(leave_kernel, n),
        name="leave",
        out_shape=(
            shape((rows, columns), F32),
            shape((8, 128), F32),
            shape((8, 128), F32),
            shape((size, features), F32),
        ),
        in_specs=[VMEM_SPEC] * 8 + [ANY_SPEC] * 2,
        out_specs=(VMEM_SPEC,) * 4,
        scratch_shapes=[
            pltpu.VMEM(normed.shape, BF16),
            pltpu.VMEM((length, features), BF16),
            pltpu.VMEM((size, features), F32),
            *PairScatter.scratch(size, features),
            *RingScatter.scratch(n, rows, columns),
            pltpu.VMEM((n, 8, 128), F32),
            pltpu.VMEM((n, 4, 8, 128), F32),
            pltpu.VMEM((n, 4, 8, 128), F32),
            pltpu.VMEM((4, 8, 128), F32),
            pltpu.VMEM((4, 8, 128), F32),
            DMA((n,)), DMA((n,)),
            DMA((n,)), DMA((n,)),
            DMA((4,)), DMA((4,)),
            DMA((2,)),
        ],
        compiler_params=pltpu.CompilerParams(collective_id=3, has_side_effects=True),
    )(cots, ctx, wqkv, x, gains, middle_cot, feed, table, normed, mixed)


def finish_kernel(
    own_ref, from_left_ref, from_right_ref, attention_ref, gain_ref, table_ref, output_in, input_in,
    gate_out, lift_out, down_out, query_out, key_out, value_out, mixer_out, gain_out, gain_two_out, table_out, output_out, input_out,
):
    hidden = gate_out.shape[1]
    heads = query_out.shape[1]
    for k, out in enumerate((gate_out, lift_out, down_out)):
        total = own_ref[k] + from_left_ref[k].astype(F32) + from_right_ref[k].astype(F32)
        out[...] = total[:, :hidden]
    for k, out in enumerate((query_out, key_out, value_out)):
        out[...] = attention_ref[...][:, k * heads : (k + 1) * heads]
    mixer_out[...] = attention_ref[...][:, 3 * heads :].T
    per = gain_out.shape[0]
    gain_out[...] = gain_ref[0:1, :per].reshape(per)
    gain_two_out[...] = gain_ref[1:2, :per].reshape(per)
    table_out[...] = table_ref[...][: table_out.shape[0], : table_out.shape[1]]
    output_out[...] = output_in[...]
    input_out[...] = input_in[...]


def finish(own, from_left, from_right, attention, gain, table, output, input_grad, hidden, heads, count, buckets, per):
    rows = own.shape[1]
    shape = jax.ShapeDtypeStruct
    square = shape((rows, heads), F32)
    return pl.pallas_call(
        finish_kernel,
        name="finish",
        out_shape=(
            *(shape((rows, hidden), F32),) * 3,
            square, square, square,
            shape((heads, rows), F32),
            shape((per,), F32),
            shape((per,), F32),
            shape((count, buckets), F32),
            shape(output.shape, F32),
            shape(input_grad.shape, F32),
        ),
        in_specs=[VMEM_SPEC] * 8,
        out_specs=(VMEM_SPEC,) * 12,
    )(own, from_left, from_right, attention, gain, table, output, input_grad)


def bucket_table(length):
    places = jnp.arange(length, dtype=jnp.int32)
    offset = places[None, :] - places[:, None]
    distance = jnp.abs(offset)
    far_bucket = 7 + sum(((distance >= limit).astype(jnp.int32) for limit in THRESHOLDS))
    near = jnp.where(distance < 8, distance, far_bucket)
    return near + jnp.where(offset > 0, 16, 0).astype(jnp.int32)


def scaled_norm(values, gain):
    return values * lax.rsqrt(jnp.mean(values * values, axis=-1, keepdims=True) + EPSILON) * gain


def gated(gate, lift):
    return jax.nn.gelu(gate, approximate=True) * lift


def dense(left, weight):
    return jnp.einsum("rld,de->rle", left, weight, preferred_element_type=jnp.float32)


def dense_back(grad, weight):
    return jnp.einsum("rle,de->rld", grad, weight, preferred_element_type=jnp.float32)


def weight_term(left, grad):
    return jnp.einsum("rld,rle->de", left, grad, preferred_element_type=jnp.float32)


def collect(part):
    return lax.all_gather(part, "mp", axis=1, tiled=True)


def spread(part):
    return lax.psum_scatter(part, "mp", scatter_dimension=1, tiled=True)


def split_heads(rows, count):
    return rows.reshape(rows.shape[0], count, rows.shape[1] // count)


def bias_blocks(table_part, buckets):
    length = buckets.shape[0]
    block = min(length, 128)
    tiles = buckets.reshape(length // block, block, length)
    codes = jnp.arange(table_part.shape[0], dtype=jnp.int32)

    def bias_one_block(tile):
        onehot = (tile[None] == codes[:, None, None]).astype(jnp.float32)
        return jnp.einsum("bij,bh->hij", onehot, table_part, precision=HIGHEST)

    pieces = lax.map(bias_one_block, tiles)
    return jnp.transpose(pieces, (1, 0, 2, 3)).reshape(table_part.shape[1], length, length)


def table_terms(score_total, buckets, count):
    heads_here, length, _ = score_total.shape
    block = min(length, 128)
    tiles = buckets.reshape(length // block, block, length)
    pieces = jnp.transpose(
        score_total.reshape(heads_here, length // block, block, length), (1, 0, 2, 3)
    )
    codes = jnp.arange(count, dtype=jnp.int32)

    def table_one_block(total, pair):
        tile, piece = pair
        onehot = (tile[None] == codes[:, None, None]).astype(jnp.float32)
        return (total + jnp.einsum("bij,hij->bh", onehot, piece, precision=HIGHEST), None)

    result, _ = lax.scan(
        table_one_block, jnp.zeros((count, heads_here), jnp.float32), (tiles, pieces)
    )
    return result


def native(
    inputs,
    segments,
    attend_gain,
    feed_gain,
    w_query,
    w_key,
    w_value,
    w_mixer,
    rel_table,
    w_gate,
    w_lift,
    w_down,
    cotangent,
):
    length = segments.shape[1]
    heads_here = rel_table.shape[1]
    buckets = bucket_table(length)
    bias = bias_blocks(rel_table, buckets)
    gains = (
        lax.all_gather(attend_gain.astype(jnp.bfloat16), ("dp", "mp"), axis=0, tiled=True),
        lax.all_gather(feed_gain.astype(jnp.bfloat16), ("dp", "mp"), axis=0, tiled=True),
    )
    first_gain = gains[0].astype(jnp.float32)
    second_gain = gains[1].astype(jnp.float32)
    attention_full = (
        lax.all_gather(w_query.astype(jnp.bfloat16), "dp", axis=0, tiled=True),
        lax.all_gather(w_key.astype(jnp.bfloat16), "dp", axis=0, tiled=True),
        lax.all_gather(w_value.astype(jnp.bfloat16), "dp", axis=0, tiled=True),
        lax.all_gather(w_mixer.astype(jnp.bfloat16), "dp", axis=1, tiled=True),
    )
    feed_full = (
        lax.all_gather(w_gate.astype(jnp.bfloat16), "dp", axis=0, tiled=True),
        lax.all_gather(w_lift.astype(jnp.bfloat16), "dp", axis=0, tiled=True),
        lax.all_gather(w_down.astype(jnp.bfloat16), "dp", axis=1, tiled=True),
    )

    def score_rows(query_heads, key_heads, segment_row):
        scores = (
            jnp.einsum("ihe,jhe->hij", query_heads, key_heads, preferred_element_type=jnp.float32)
            + bias
        )
        same = segment_row[:, None] == segment_row[None, :]
        return jnp.where(same[None], scores, MASKED)

    normed = scaled_norm(inputs, first_gain).astype(jnp.bfloat16)
    normed_full = collect(normed)
    query = dense(normed_full, attention_full[0]).astype(jnp.bfloat16)
    keys = dense(normed_full, attention_full[1]).astype(jnp.bfloat16)
    values = dense(normed_full, attention_full[2]).astype(jnp.bfloat16)

    def attend(row):
        query_row, key_row, value_row, segment_row = row
        query_heads = split_heads(query_row, heads_here)
        key_heads = split_heads(key_row, heads_here)
        value_heads = split_heads(value_row, heads_here)
        scores = score_rows(query_heads, key_heads, segment_row)
        largest = jnp.max(scores, axis=-1, keepdims=True)
        raised = jnp.exp(scores - largest)
        totals = jnp.sum(raised, axis=-1, keepdims=True)
        probs = (raised / totals).astype(jnp.bfloat16)
        context = jnp.einsum("hij,jhe->ihe", probs, value_heads, preferred_element_type=jnp.float32)
        return (
            context.astype(jnp.bfloat16).reshape(length, -1),
            (largest + jnp.log(totals))[..., 0],
        )

    context, logsum = lax.map(attend, (query, keys, values, segments))
    middle = inputs + spread(dense(context, attention_full[3]))
    normed_two = scaled_norm(middle, second_gain).astype(jnp.bfloat16)
    second_full = collect(normed_two)
    gate = dense(second_full, feed_full[0])
    lift = dense(second_full, feed_full[1])
    hidden = gated(gate, lift).astype(jnp.bfloat16)
    output = middle + spread(dense(hidden, feed_full[2]))
    feed_back = (
        lax.all_gather(w_gate.astype(jnp.bfloat16), "dp", axis=0, tiled=True),
        lax.all_gather(w_lift.astype(jnp.bfloat16), "dp", axis=0, tiled=True),
        lax.all_gather(w_down.astype(jnp.bfloat16), "dp", axis=1, tiled=True),
    )
    down_full = collect(cotangent.astype(jnp.bfloat16))
    hidden_cot = dense_back(down_full, feed_back[2])
    down_term = weight_term(hidden, down_full)
    _, gated_pull = jax.vjp(gated, gate, lift)
    gate_cot, lift_cot = gated_pull(hidden_cot)
    gate_cot = gate_cot.astype(jnp.bfloat16)
    lift_cot = lift_cot.astype(jnp.bfloat16)
    gate_term = weight_term(second_full, gate_cot)
    lift_term = weight_term(second_full, lift_cot)
    second_cot = spread(dense_back(gate_cot, feed_back[0]) + dense_back(lift_cot, feed_back[1]))
    _, second_pull = jax.vjp(scaled_norm, middle, second_gain)
    middle_from_norm, second_gain_term = second_pull(second_cot)
    middle_cot = cotangent + middle_from_norm
    attention_back = (
        lax.all_gather(w_query.astype(jnp.bfloat16), "dp", axis=0, tiled=True),
        lax.all_gather(w_key.astype(jnp.bfloat16), "dp", axis=0, tiled=True),
        lax.all_gather(w_value.astype(jnp.bfloat16), "dp", axis=0, tiled=True),
        lax.all_gather(w_mixer.astype(jnp.bfloat16), "dp", axis=1, tiled=True),
    )
    mixed_full = collect(middle_cot.astype(jnp.bfloat16))
    context_cot = dense_back(mixed_full, attention_back[3]).astype(jnp.bfloat16)
    mixer_term = weight_term(context, mixed_full)

    def attend_back(total, row):
        query_row, key_row, value_row, segment_row, log_row, cot_row = row
        query_heads = split_heads(query_row, heads_here)
        key_heads = split_heads(key_row, heads_here)
        value_heads = split_heads(value_row, heads_here)
        cot_heads = split_heads(cot_row, heads_here)
        scores = score_rows(query_heads, key_heads, segment_row)
        probs = jnp.exp(scores - log_row[:, :, None])
        value_cot = jnp.einsum(
            "hij,ihe->jhe",
            probs.astype(jnp.bfloat16),
            cot_heads,
            preferred_element_type=jnp.float32,
        )
        prob_cot = jnp.einsum(
            "ihe,jhe->hij", cot_heads, value_heads, preferred_element_type=jnp.float32
        )
        inner = jnp.sum(probs * prob_cot, axis=-1, keepdims=True)
        score_cot = (probs * (prob_cot - inner)).astype(jnp.bfloat16)
        query_cot = jnp.einsum(
            "hij,jhe->ihe", score_cot, key_heads, preferred_element_type=jnp.float32
        )
        key_cot = jnp.einsum(
            "hij,ihe->jhe", score_cot, query_heads, preferred_element_type=jnp.float32
        )
        outputs = (
            query_cot.astype(jnp.bfloat16).reshape(length, -1),
            key_cot.astype(jnp.bfloat16).reshape(length, -1),
            value_cot.astype(jnp.bfloat16).reshape(length, -1),
        )
        return (total + score_cot.astype(jnp.float32), outputs)

    score_total, cots = lax.scan(
        attend_back,
        jnp.zeros((heads_here, length, length), jnp.float32),
        (query, keys, values, segments, logsum, context_cot),
    )
    query_cot, key_cot, value_cot = cots
    query_term = weight_term(normed_full, query_cot)
    key_term = weight_term(normed_full, key_cot)
    value_term = weight_term(normed_full, value_cot)
    first_cot = spread(
        dense_back(query_cot, attention_back[0])
        + dense_back(key_cot, attention_back[1])
        + dense_back(value_cot, attention_back[2])
    )
    _, first_pull = jax.vjp(scaled_norm, inputs, first_gain)
    input_from_norm, first_gain_term = first_pull(first_cot)
    input_grad = middle_cot + input_from_norm
    table_grad = lax.psum(table_terms(score_total, buckets, rel_table.shape[0]), "dp")
    gain_grads = (
        lax.psum_scatter(first_gain_term, ("dp", "mp"), scatter_dimension=0, tiled=True),
        lax.psum_scatter(second_gain_term, ("dp", "mp"), scatter_dimension=0, tiled=True),
    )
    summed = (
        lax.psum_scatter(query_term, "dp", scatter_dimension=0, tiled=True),
        lax.psum_scatter(key_term, "dp", scatter_dimension=0, tiled=True),
        lax.psum_scatter(value_term, "dp", scatter_dimension=0, tiled=True),
        lax.psum_scatter(mixer_term, "dp", scatter_dimension=1, tiled=True),
        lax.psum_scatter(gate_term, "dp", scatter_dimension=0, tiled=True),
        lax.psum_scatter(lift_term, "dp", scatter_dimension=0, tiled=True),
        lax.psum_scatter(down_term, "dp", scatter_dimension=1, tiled=True),
    )
    return (
        output,
        input_grad,
        gain_grads[0],
        gain_grads[1],
        summed[0],
        summed[1],
        summed[2],
        summed[3],
        table_grad,
        summed[4],
        summed[5],
        summed[6],
    )


def ring_order(n):
    return [2 * p if p < n // 2 else 2 * (n - 1 - p) + 1 for p in range(n)]


def to_neighbours(n, right, left):
    ring = ring_order(n)
    onward = [(ring[p], ring[(p + 1) % n]) for p in range(n)]
    return lax.ppermute(right, "dp", onward), lax.ppermute(left, "dp", [(b, a) for a, b in onward])


def fused(
    n,
    inputs,
    segments,
    attend_gain,
    feed_gain,
    w_query,
    w_key,
    w_value,
    w_mixer,
    rel_table,
    w_gate,
    w_lift,
    w_down,
    cotangent,
):
    x, cot = inputs[0], cotangent[0]
    normed, cots, gate_full, qkv, wqkv, wmix, tiles, lift, down, gains = enter(
        n, x, cot, attend_gain, feed_gain, w_query, w_key, w_value, w_mixer, w_gate, w_lift, w_down.T, rel_table.T
    )
    from_left, from_right = to_neighbours(n, lift, lift)
    context, context32, logsum = attend(qkv, segments, tiles)
    second, lift_full, down_full, bend, slope, hidden, middle = middle_part(
        n, context, wmix, x, gains, lift, from_left, from_right, down, gate_full
    )
    mixed, pending, output, middle_cot, feed, own = back_part(
        n, middle, cot, gains, hidden, cots, second, bend, slope, gate_full, lift_full, down_full
    )
    sums_left, sums_right = to_neighbours(n, pending[0], pending[1])
    qkv_cot, table = attend_back(qkv, segments, tiles, context32, logsum, mixed, wmix)
    attention_term, gain_term, table_term, input_grad = leave_part(
        n, qkv_cot, context, wqkv, x, gains, middle_cot, feed, table, normed, mixed
    )
    gate_grad, lift_grad, down_grad, query_grad, key_grad, value_grad, mixer_grad, first, second, table_grad, output, input_grad = finish(
        own, sums_left, sums_right, attention_term, gain_term, table_term, output, input_grad,
        w_gate.shape[1], w_query.shape[1], rel_table.shape[1], rel_table.shape[0], attend_gain.shape[0],
    )
    return (
        output[None],
        input_grad[None],
        first,
        second,
        query_grad,
        key_grad,
        value_grad,
        mixer_grad,
        table_grad.T,
        gate_grad,
        lift_grad,
        down_grad.T,
    )


def layer(mesh, inputs, *rest):
    n, pairs = mesh.shape["dp"], mesh.shape["mp"]
    tokens, hidden = inputs.shape[1] * pairs, rest[8].shape[1]
    slots = inputs.shape[2] // n
    if n == 8 and pairs == 4 and slots % 64 == 0 and hidden + -hidden % 128 == tokens and tokens % BLOCK == 0:
        return fused(n, inputs, *rest)
    return native(inputs, *rest)


def solution(mesh):
    return jax.shard_map(
        functools.partial(layer, mesh),
        mesh=mesh,
        in_specs=(
            P("dp", "mp", None),
            P("dp", None),
            P(("dp", "mp")),
            P(("dp", "mp")),
            P("dp", "mp"),
            P("dp", "mp"),
            P("dp", "mp"),
            P("mp", "dp"),
            P(None, "mp"),
            P("dp", "mp"),
            P("dp", "mp"),
            P("mp", "dp"),
            P("dp", "mp", None),
        ),
        out_specs=(
            P("dp", "mp", None),
            P("dp", "mp", None),
            P(("dp", "mp")),
            P(("dp", "mp")),
            P("dp", "mp"),
            P("dp", "mp"),
            P("dp", "mp"),
            P("mp", "dp"),
            P(None, "mp"),
            P("dp", "mp"),
            P("dp", "mp"),
            P("mp", "dp"),
        ),
        check_vma=False,
    )
```
